256 devices in a mesh: gx: 64 (over x, z, core), gy: 4 (over y).
Axes of the slice: x: 4, y: 4, z: 8, core: 2. Of those that a mesh axis runs over, the one named last changes fastest.
Arguments:
- measures: bfloat16 [2097152, 128], P(('gx', 'gy')), may hold values from -6 to 6
- row_keys: int32 [2097152], P(('gx', 'gy')), may hold values from 0 to 131071, as said below
- orders: bfloat16 [131072, 128], P(('gx', 'gy')), may hold values from -6 to 6
- heavy_keys: int32 [512], replicated, may hold values from 0 to 131071, as said below
- key_slot: int32 [131072], replicated, may hold values from 0 to 131071, as said below
Outputs:
- result: bfloat16 [131072, 128], P(('gx', 'gy'))
- heavy_report: bfloat16 [512, 128], P(('gx', 'gy'))
- slot_rows: float32 [131072], P(('gx', 'gy'))
The draws below stay inside these ranges and needn't reach their ends.
Inputs may be any that keep to these rules, and one draw needn't show every extreme that they name: `heavy_keys`: for each range block d, entries d * 2 to (d + 1) * 2 - 1 are distinct keys of d * 512 to (d + 1) * 512 - 1. `key_slot`: A permutation. Slot s belongs to owner s // 2048 and to quarter (s // 512) % q with q = 4. Key k lies in range block d = k // 512; every range block has exactly 8 keys with slots of each owner, all in quarter d % q. `row_keys`: in the rows of one device, among rows whose key is not heavy, at most 256 have slots of any one owner and at most 64 distinct keys have slots of any one owner; in every device both bounds are reached by some owner.
All inputs are finite; a program needn't handle non-finite values.
Results may differ from the reference program's by a relative error of at most 0.0021.
Values may be sent and summed in bfloat16 or wider, within the bound.
A program may use at most 64 MiB of HBM per device.

```python
import jax
import jax.numpy as jnp
from jax import lax

W = 128
ROWS_DEV = 8192
KEY_DEV = 512
HPD = 2
ROWS = 2097152
KEYS = 131072
HEAVY = 512
OWN_SLOTS = 2048
KPP = 8
CAP = 256
CAPK = 64
N_GX = 64
N_GY = 4
DEVICES = 256


def layout(base):
    seeded = jax.random.fold_in(base, 7)
    first, second, third = jax.random.split(seeded, 3)
    owner_perm = jax.vmap(lambda keyone: jax.random.permutation(keyone, KEY_DEV))(jax.random.split(first, DEVICES))
    device = jnp.arange(DEVICES, dtype=jnp.int32)
    along_x = device // N_GY
    along_y = device % N_GY
    owners = owner_perm // KPP
    within = owner_perm % KPP
    shuffle = jax.vmap(lambda keyone: jax.random.permutation(keyone, KEY_DEV))(jax.random.split(second, N_GX * N_GY))
    shuffle = shuffle.reshape(N_GX, N_GY, KEY_DEV)
    position = shuffle[owners, along_y[:, None], along_x[:, None] * KPP + within]
    key_slot = ((owners * N_GY + along_y[:, None]) * KEY_DEV + position).reshape(KEYS).astype(jnp.int32)
    picked = jax.vmap(lambda keyone: jax.random.permutation(keyone, KEY_DEV)[:HPD])(jax.random.split(third, DEVICES))
    heavy_keys = (device[:, None] * KEY_DEV + picked).reshape(HEAVY).astype(jnp.int32)
    slot_to_key = jnp.argsort(key_slot).astype(jnp.int32)
    heavy_flag = jnp.zeros((KEYS,), jnp.int32).at[heavy_keys].set(1)
    heavy_slot = heavy_flag[slot_to_key]
    return (key_slot, heavy_keys, slot_to_key, heavy_slot)


def draw_key_slot(key, part):
    return layout(key)[0]


def draw_heavy_keys(key, part):
    return layout(key)[1]


def draw_row_keys(key, part):
    key_slot, heavy_keys, slot_to_key, heavy_slot = layout(key)
    seeded = jax.random.fold_in(key, 11)
    favored_pool = jax.random.permutation(jax.random.fold_in(seeded, 3), N_GX)[:max(1, N_GX // 16)]
    tickets = N_GX * CAP
    pool_rank = jnp.where(heavy_slot.reshape(N_GX, OWN_SLOTS) == 1, OWN_SLOTS, 0)

    def one_device(keyone):
        parts = jax.random.split(keyone, 7)
        heavy_count = jax.random.randint(parts[0], (), ROWS_DEV // 4, ROWS_DEV // 2 + 1)
        light_count = ROWS_DEV - heavy_count
        favored = favored_pool[jax.random.randint(parts[1], (), 0, favored_pool.shape[0])]
        ticket_owner = jnp.arange(tickets, dtype=jnp.int32) // CAP
        scores = jnp.where(ticket_owner == favored, 0, tickets) + jax.random.permutation(parts[2], tickets)
        ticket_order = jnp.argsort(scores).astype(jnp.int32)
        row_index = jnp.arange(ROWS_DEV, dtype=jnp.int32)
        chosen = ticket_order[jnp.minimum(row_index, tickets - 1)]
        row_owner = chosen // CAP
        row_ticket = chosen % CAP
        mixing = jax.vmap(lambda keytwo: jax.random.permutation(keytwo, OWN_SLOTS))(jax.random.split(parts[3], N_GX))
        pools = jnp.argsort(pool_rank + mixing, axis=1)[:, :CAPK].astype(jnp.int32)
        spare = jax.random.randint(parts[4], (ROWS_DEV,), 0, CAPK)
        pool_index = jnp.where(row_ticket < CAPK, row_ticket, spare)
        light_keys = slot_to_key[row_owner * OWN_SLOTS + pools[row_owner, pool_index]]
        heavy_pick = heavy_keys[jax.random.randint(parts[5], (ROWS_DEV,), 0, HEAVY)]
        chosen_keys = jnp.where(row_index < light_count, light_keys, heavy_pick)
        return chosen_keys[jax.random.permutation(parts[6], ROWS_DEV)]
    return jax.vmap(one_device)(jax.random.split(seeded, DEVICES)).reshape(ROWS).astype(jnp.int32)


def level_of(own_key, dims, cuts, least, largest):
    factor_of = 1.0
    for dim, shards_of in cuts:
        draws = jax.random.uniform(jax.random.fold_in(jax.random.fold_in(own_key, 6), dim), (shards_of,), jnp.float32, least / len(cuts), largest / len(cuts))
        factor_of = factor_of * jnp.repeat(jnp.exp(draws), dims[dim] // shards_of).reshape((-1,) + (1,) * (len(dims) - 1 - dim))
    return factor_of


def scatter_about(rng, dims, spread, reach, pieces=(), kind=jnp.bfloat16):
    gain = level_of(rng, dims, pieces, -0.22, 0.18) if pieces else 1.0
    drawn = jax.random.normal(rng, dims, jnp.float32) * spread * gain
    return jnp.minimum(jnp.maximum(drawn, -reach), reach).astype(kind)


def setup_inputs(seed: int = 0) -> dict:
    key_list = jax.random.split(jax.random.key(seed), 6)
    return {
        "measures": scatter_about(key_list[0], (ROWS, W), 1.0, 6.0, ((0, 256),)),
        "row_keys": draw_row_keys(jax.random.fold_in(key_list[5], 71), 0),
        "orders": scatter_about(key_list[2], (KEYS, W), 1.0, 6.0, ((0, 256),)),
        "heavy_keys": draw_heavy_keys(jax.random.fold_in(key_list[5], 71), 0),
        "key_slot": draw_key_slot(jax.random.fold_in(key_list[5], 71), 0),
    }


def reference(measures, row_keys, orders, heavy_keys, key_slot):
    blocks = measures.reshape(DEVICES, ROWS_DEV, W)
    block_keys = row_keys.reshape(DEVICES, ROWS_DEV)

    def add_block(running, block_piece):
        block_rows, keys_here = block_piece
        totals = running[0] + jax.ops.segment_sum(block_rows.astype(jnp.float32), keys_here, num_segments=KEYS)
        tallies = running[1] + jax.ops.segment_sum(jnp.ones((ROWS_DEV,), jnp.float32), keys_here, num_segments=KEYS)
        return ((totals, tallies), None)
    start_state = (jnp.zeros((KEYS, W), jnp.float32), jnp.zeros((KEYS,), jnp.float32))
    (sums, counts), unused = lax.scan(add_block, start_state, (blocks, block_keys))
    joined = orders.astype(jnp.float32) * sums * lax.rsqrt(1.0 + counts)[:, None]
    result = joined.astype(jnp.bfloat16)
    heavy_report = joined[heavy_keys].astype(jnp.bfloat16)
    heavy_flag = jnp.zeros((KEYS,), jnp.float32).at[heavy_keys].set(1.0)
    slot_rows = jnp.zeros((KEYS,), jnp.float32).at[key_slot].set(counts * (1.0 - heavy_flag))
    return (result, heavy_report, slot_rows)
```

```python
import functools

import jax
import jax.numpy as jnp
from jax import lax
from jax.experimental import pallas as pl
from jax.experimental.pallas import tpu as pltpu
from jax.sharding import PartitionSpec as P

MESH = pl.DeviceIdType.MESH
F32, BF16, I32, I16 = jnp.float32, jnp.bfloat16, jnp.int32, jnp.int16
LN2 = 0.6931471805599453

W = 128
GX, GY = 64, 4
KEYS = 131072
KD = 512
OWN = 2048
CAPK = 64
HG = 8
MSG = 80
LANES = 1024
VMEM = pl.BlockSpec(memory_space=pltpu.VMEM)


def iota(shape, dim):
    return lax.broadcasted_iota(I32, shape, dim)


def onehot(rows, lanes, base, labels):
    return jnp.where(iota((rows, lanes), 0) + base == labels, 1.0, 0.0).astype(BF16)


def dot(a, b):
    return jnp.dot(a, b, preferred_element_type=F32)


def dot_t(a, b):
    return lax.dot_general(a, b, (((1,), (1,)), ((), ())), preferred_element_type=F32)


def power(e):
    return jnp.exp(e * LN2)


def encode(v):
    top = jnp.max(jnp.abs(v), axis=1, keepdims=True)
    e = jnp.ceil(jnp.log(jnp.maximum(top, 1e-30)) * (1.0 / LN2) - 14.99)
    e = jnp.maximum(e, -100.0)
    q = jnp.floor(v * power(-e) + 0.5).astype(I32)
    return q, e


def gather_kernel(keys_ref, x_ref, ks_ref, hk_ref, msg_ref,
                  tab, shi_s, slo_s, seg_s, xe, pt, rk, acc, hq, hx):
    chunks = keys_ref.shape[0]
    hi_n, lo_n = ks_ref.shape
    ks = ks_ref[...]
    key_id = iota((hi_n, lo_n), 0) * lo_n + iota((hi_n, lo_n), 1)
    p1 = (ks >> 11) * 2 + ((ks >> 8) & 1)
    p1 = jnp.where(key_id == hk_ref[:, 0:1], 128, p1)
    p1 = jnp.where(key_id == hk_ref[:, 1:2], 129, p1)
    p2 = ks & 255
    tab[0:lo_n, :] = p1.astype(F32).T.astype(BF16)
    tab[lo_n : 2 * lo_n, :] = p2.astype(F32).T.astype(BF16)
    pt[...] = jnp.zeros_like(pt)

    def look(c, carry):
        key = keys_ref[pl.ds(c, 1), :]
        hi, lo = key >> 8, key & 255
        t = dot(tab[...], onehot(hi_n, LANES, 0, hi))
        mine = iota((lo_n, LANES), 0) == lo
        a = jnp.sum(jnp.where(mine, t[:lo_n], 0.0), axis=0, keepdims=True).astype(I32)
        b = jnp.sum(jnp.where(mine, t[lo_n:], 0.0), axis=0, keepdims=True).astype(I32)
        heavy = a >= 128
        shi = jnp.where(heavy, -1, (a >> 1) * 8 + ((key >> 9) & 3) * 2 + (a & 1))
        shi_s[pl.ds(c, 1), :] = shi
        slo_s[pl.ds(c, 1), :] = b
        seg_s[pl.ds(c, 1), :] = jnp.where(
            heavy, GX * CAPK + (key >> 9) * 2 + (a - 128), (a >> 1) * CAPK
        )
        pt[...] += dot_t(onehot(lo_n, LANES, 0, b), onehot(hi_n, LANES, 0, shi))
        return carry

    lax.fori_loop(0, chunks, look, 0)

    here = jnp.where(pt[...] > 0.5, 1.0, 0.0).astype(BF16)
    lower = jnp.where(iota((lo_n, lo_n), 1) < iota((lo_n, lo_n), 0), 1.0, 0.0).astype(BF16)
    r0, r1 = iota((hi_n, hi_n), 0), iota((hi_n, hi_n), 1)
    before = jnp.where((r0 < r1) & ((r0 >> 3) == (r1 >> 3)), 1.0, 0.0).astype(BF16)
    column = dot(jnp.ones((lo_n, lo_n), BF16), here).astype(BF16)
    rk[...] = (dot(lower, here) + dot(column, before)).astype(BF16)

    def rank(c, carry):
        shi = shi_s[pl.ds(c, 1), :]
        slo = slo_s[pl.ds(c, 1), :]
        t = dot(rk[...], onehot(hi_n, LANES, 0, shi))
        mine = iota((lo_n, LANES), 0) == slo
        r = jnp.sum(jnp.where(mine, t, 0.0), axis=0, keepdims=True).astype(I32)
        seg_s[pl.ds(c, 1), :] = seg_s[pl.ds(c, 1), :] + jnp.where(shi < 0, 0, r)
        line = iota((W, LANES), 0)
        ext = jnp.where(line == 0, 1, jnp.where(line == 1, slo, jnp.where(line == 2, shi & 7, 0)))
        at = pl.ds(pl.multiple_of(c * LANES, LANES), LANES)
        xe[at, 0:W] = x_ref[at, :]
        xe[at, W : 2 * W] = ext.astype(F32).T.astype(BF16)
        return carry

    lax.fori_loop(0, chunks, rank, 0)

    def sums(base):
        acc[...] = jnp.zeros_like(acc)

        def step(c, carry):
            at = pl.ds(pl.multiple_of(c * LANES, LANES), LANES)
            acc[...] += dot(onehot(512, LANES, base, seg_s[pl.ds(c, 1), :]), xe[at, :])
            return carry

        lax.fori_loop(0, chunks, step, 0)
        return acc[:, 0:W], acc[:, W : 2 * W]

    lane = iota((512, W), 1)
    v, ext = sums(GX * CAPK)
    q, e = encode(v)
    hq[...] = q
    hx[...] = jnp.where(lane == 64, ext[:, 0:1], jnp.where(lane == 65, e, 0.0)).astype(I32)

    def owners(m, carry):
        v, ext = sums(m * 512)
        q, e = encode(v)
        t = jnp.where(lane == 3, e, ext).T[0:8]
        cnt = t[0:1]
        slot = jnp.where(
            cnt > 0.5, jnp.floor((t[1:2] + 256.0 * t[2:3]) / jnp.maximum(cnt, 1.0) + 0.5), -1.0
        )
        line = iota((8, 512), 0)
        meta = jnp.where(line == 0, slot, jnp.where(line == 1, cnt, t[3:4])).astype(I32)
        for i in range(8):
            o = m * 8 + i
            part = meta[:, (i // 2) * W : (i // 2 + 1) * W]
            if i % 2:
                part = pltpu.roll(part, 64, 1)
            at = pl.ds(pl.multiple_of(o * 8, 8), 8)
            part = jnp.where(iota((8, W), 1) < 64, part, hx[at, :])
            msg_ref[pl.ds(o, 1), 0:64, :] = q[i * 64 : (i + 1) * 64].astype(I16)[None]
            tail = jnp.concatenate([hq[at, :], part], axis=0)
            msg_ref[pl.ds(o, 1), 64:80, :] = tail.astype(I16)[None]
        return carry

    lax.fori_loop(0, GX // 8, owners, 0)


def gather(keys, x, ks, hk):
    rows = x.shape[0]
    chunks = rows // LANES
    return pl.pallas_call(
        gather_kernel,
        out_shape=jax.ShapeDtypeStruct((GX, MSG, W), I16),
        in_specs=[VMEM] * 4,
        out_specs=VMEM,
        scratch_shapes=[
            pltpu.VMEM((512, 512), BF16),
            pltpu.VMEM((chunks, LANES), I32),
            pltpu.VMEM((chunks, LANES), I32),
            pltpu.VMEM((chunks, LANES), I32),
            pltpu.VMEM((rows, 2 * W), BF16),
            pltpu.VMEM((256, 512), F32),
            pltpu.VMEM((256, 512), BF16),
            pltpu.VMEM((512, 2 * W), F32),
            pltpu.VMEM((512, W), I32),
            pltpu.VMEM((512, W), I32),
        ],
        compiler_params=pltpu.CompilerParams(vmem_limit_bytes=50 * 2**20),
        name="gather_rows",
    )(keys, x, ks, hk)


def peer_gx(me, k):
    core, z, x = me % 2, (me // 2) % 8, me // 16
    j = k // 2
    zi, dx = j // 4, j % 4
    dz = ((zi + 1) // 2) * (1 - 2 * ((zi + 1) % 2))
    return (((x + dx) % 4) * 8 + (z + 8 + dz) % 8) * 2 + (core + k) % 2


def source_gx(me, k):
    core, z, x = me % 2, (me // 2) % 8, me // 16
    j = k // 2
    zi, dx = j // 4, j % 4
    dz = ((zi + 1) // 2) * (1 - 2 * ((zi + 1) % 2))
    return (((x + 4 - dx) % 4) * 8 + (z + 8 - dz) % 8) * 2 + (core + k) % 2


def peer_ring(n, me, k):
    return (me + k) % n


def source_ring(n, me, k):
    return (me + n - k) % n


def exchange_kernel(axis, n, to, frm, x_ref, o_ref, ssem, rsem, lsem):
    me = lax.axis_index(axis)
    barrier = pltpu.get_barrier_semaphore()

    def greet(k, carry):
        pl.semaphore_signal(barrier, inc=1, device_id={axis: to(me, k)}, device_id_type=MESH)
        return carry

    lax.fori_loop(1, n, greet, 0)
    own = pltpu.make_async_copy(x_ref.at[me], o_ref.at[me], lsem)
    own.start()
    pl.semaphore_wait(barrier, n - 1)

    def send(k, carry):
        p = to(me, k)
        pltpu.make_async_remote_copy(
            src_ref=x_ref.at[p], dst_ref=o_ref.at[me], send_sem=ssem.at[p], recv_sem=rsem.at[me],
            device_id={axis: p}, device_id_type=MESH,
        ).start()
        return carry

    lax.fori_loop(1, n, send, 0)
    own.wait()

    def finish(k, carry):
        p, s = to(me, k), frm(me, k)
        pltpu.make_async_remote_copy(
            src_ref=x_ref.at[p], dst_ref=o_ref.at[s], send_sem=ssem.at[p], recv_sem=rsem.at[s],
            device_id={axis: p}, device_id_type=MESH,
        ).wait()
        return carry

    lax.fori_loop(1, n, finish, 0)


def exchange(x, axis, n, to, frm, cid):
    return pl.pallas_call(
        functools.partial(exchange_kernel, axis, n, to, frm),
        out_shape=jax.ShapeDtypeStruct(x.shape, x.dtype),
        in_specs=[VMEM],
        out_specs=VMEM,
        scratch_shapes=[
            pltpu.SemaphoreType.DMA((n,)),
            pltpu.SemaphoreType.DMA((n,)),
            pltpu.SemaphoreType.DMA,
        ],
        compiler_params=pltpu.CompilerParams(
            collective_id=cid, has_side_effects=True, vmem_limit_bytes=32 * 2**20
        ),
        name="exchange_" + axis + str(cid),
    )(x)


def slots_of(ks, me):
    mine = jnp.where((ks >> 11) == me, 1.0, 0.0)
    upper = jnp.where(iota((KD, KD), 0) < iota((KD, KD), 1), 1.0, 0.0).astype(BF16)
    w = dot(mine.astype(BF16), upper)
    pos = (ks & (KD - 1)).astype(F32)
    lane = iota((GX, W), 1)
    table = jnp.zeros((GX, W), F32)
    for k in range(8):
        s = jnp.sum(jnp.where((mine > 0.5) & (w == float(k)), pos, 0.0), axis=1, keepdims=True)
        table = jnp.where(lane == k, s, table)
    high = jnp.floor(table * (1.0 / 256.0))
    low = table - 256.0 * high
    repeat = jnp.where((iota((KD, GX), 0) >> 3) == iota((KD, GX), 1), 1.0, 0.0).astype(BF16)
    each = 256.0 * dot(repeat, high.astype(BF16)) + dot(repeat, low.astype(BF16))
    pick = iota((KD, W), 1) == (iota((KD, W), 0) & 7)
    return jnp.sum(jnp.where(pick, each, 0.0), axis=1, keepdims=True).astype(I32)


def owner_kernel(msg_ref, ks_ref, out_ref, v_s, meta_s, scol, acc, tal, heavy, hcount):
    me = lax.axis_index("gx")
    for q in range(GY):
        scol[q * KD : (q + 1) * KD, :] = slots_of(ks_ref[:, q * KD : (q + 1) * KD], me) + q * KD
    heavy[...] = jnp.zeros_like(heavy)
    hcount[...] = jnp.zeros_like(hcount)
    lane = iota((8, W), 1)

    def unpack(p, carry):
        metas = []
        for i in range(2):
            s = 2 * p + i
            q = msg_ref[pl.ds(s, 1), 0:64, :][0].astype(I32)
            at = pl.ds(pl.multiple_of(s * 64, 64), 64)
            high = q >> 8
            v_s[at, 0:W] = high.astype(F32).astype(BF16)
            v_s[at, W : 2 * W] = (q - high * 256).astype(F32).astype(BF16)
            tail = msg_ref[pl.ds(s, 1), 64:80, :][0].astype(I32)
            meta = tail[8:16]
            heavy[...] += tail[0:8].astype(F32) * power(meta[:, 65:66].astype(F32))
            hcount[...] += meta[:, 64:65].astype(F32) + jnp.zeros((8, W), F32)
            metas.append(meta)
        both = jnp.where(lane < 64, metas[0], pltpu.roll(metas[1], 64, 1))
        meta_s[:, pl.ds(pl.multiple_of(p * W, W), W)] = both
        return carry

    lax.fori_loop(0, GX // 2, unpack, 0)

    def quarter(q, carry):
        acc[...] = jnp.zeros_like(acc)
        tal[...] = jnp.zeros_like(tal)
        labels = scol[pl.ds(pl.multiple_of(q * KD, KD), KD), :]

        def step(c, carry):
            at = pl.ds(pl.multiple_of(c * LANES, LANES), LANES)
            meta = meta_s[:, at]
            mine = labels == meta[0:1]
            scale = power(meta[2:3].astype(F32))
            oh = jnp.where(mine, scale, 0.0).astype(BF16)
            acc[...] += dot(oh, v_s[at, :])
            hits = jnp.where(mine, meta[1:2].astype(F32), 0.0)
            t = hits[:, 0:W]
            for i in range(1, LANES // W):
                t = t + hits[:, i * W : (i + 1) * W]
            tal[...] += t
            return carry

        lax.fori_loop(0, GX * CAPK // LANES, step, 0)
        out_ref[pl.ds(q, 1), 0:KD, :] = (acc[:, 0:W] * 256.0 + acc[:, W : 2 * W])[None]
        t = jnp.sum(tal[...].T, axis=0, keepdims=True)
        line = iota((8, W), 0)
        rows = jnp.zeros((8, W), F32)
        for i in range(4):
            rows = jnp.where(line == i, t[:, i * W : (i + 1) * W], rows)
        out_ref[pl.ds(q, 1), KD : KD + 8, :] = rows[None]
        return carry

    lax.fori_loop(0, GY, quarter, 0)
    line = iota((8, W), 0)
    for q in range(GY):
        rows = jnp.where(line == 0, heavy[2 * q : 2 * q + 1], 0.0)
        rows = jnp.where(line == 1, heavy[2 * q + 1 : 2 * q + 2], rows)
        rows = jnp.where(line == 2, hcount[2 * q : 2 * q + 1], rows)
        rows = jnp.where(line == 3, hcount[2 * q + 1 : 2 * q + 2], rows)
        out_ref[q, KD + 8 : KD + 16, :] = rows


def owner(msg, ks):
    return pl.pallas_call(
        owner_kernel,
        out_shape=jax.ShapeDtypeStruct((GY, KD + 16, W), F32),
        in_specs=[VMEM] * 2,
        out_specs=VMEM,
        scratch_shapes=[
            pltpu.VMEM((GX * CAPK, 2 * W), BF16),
            pltpu.VMEM((8, GX * CAPK), I32),
            pltpu.VMEM((OWN, 1), I32),
            pltpu.VMEM((KD, 2 * W), F32),
            pltpu.VMEM((KD, W), F32),
            pltpu.VMEM((8, W), F32),
            pltpu.VMEM((8, W), F32),
        ],
        compiler_params=pltpu.CompilerParams(vmem_limit_bytes=50 * 2**20),
        name="owner_sums",
    )(msg, ks)


def quarter_kernel(got_ref, ks_ref, out_ref, slots_ref, heavy_ref):
    me = lax.axis_index("gx")
    total = got_ref[0] + got_ref[1] + got_ref[2] + got_ref[3]
    counts = total[KD : KD + 8]
    square = jnp.concatenate([counts, jnp.zeros((W - 8, W), F32)], axis=0).T
    column = jnp.concatenate([square[:, i : i + 1] for i in range(4)], axis=0)
    out_ref[...] = total[0:KD] * lax.rsqrt(1.0 + column)
    pos = slots_of(ks_ref[...], me)
    slots_ref[...] = jnp.sum(
        jnp.where(pos == iota((KD, KD), 1), column, 0.0), axis=0, keepdims=True
    )
    tail = total[KD + 8 : KD + 16]
    heavy_ref[...] = tail * lax.rsqrt(1.0 + pltpu.roll(tail, 6, 0))


def quarter(got, ks):
    return pl.pallas_call(
        quarter_kernel,
        out_shape=(
            jax.ShapeDtypeStruct((KD, W), F32),
            jax.ShapeDtypeStruct((1, KD), F32),
            jax.ShapeDtypeStruct((8, W), F32),
        ),
        in_specs=[VMEM] * 2,
        out_specs=(VMEM,) * 3,
        compiler_params=pltpu.CompilerParams(vmem_limit_bytes=32 * 2**20),
        name="quarter_totals",
    )(got, ks)


def result_kernel(got_ref, orders_ref, row_ref, col_ref, hloc_ref, heavy_ref, out_ref, report_ref):
    own_row = row_ref[...] >> 11
    own_col = col_ref[...] >> 11
    j0, j1 = iota((KD, KD), 0), iota((KD, KD), 1)
    w = jnp.sum(jnp.where((own_row == own_col) & (j1 < j0), 1.0, 0.0), axis=1, keepdims=True)
    place = own_col * 8 + w.astype(I32)
    oh = jnp.where(place == j1, 1.0, 0.0).astype(BF16)
    got = got_ref[...]
    high = got.astype(BF16)
    low = (got - high.astype(F32)).astype(BF16)
    total = dot(oh, high) + dot(oh, low)
    orders = orders_ref[...].astype(F32)
    line = iota((KD, W), 0)
    reports = []
    for h in range(2):
        here = line == hloc_ref[h]
        total = jnp.where(here, heavy_ref[h : h + 1, :], total)
        mine = jnp.sum(jnp.where(here, orders, 0.0), axis=0, keepdims=True)
        reports.append(mine * heavy_ref[h : h + 1, :])
    out_ref[...] = (orders * total).astype(BF16)
    report_ref[...] = jnp.concatenate(reports, axis=0).astype(BF16)


def outputs(got, orders, row, col, hloc, heavy):
    return pl.pallas_call(
        result_kernel,
        out_shape=(jax.ShapeDtypeStruct((KD, W), BF16), jax.ShapeDtypeStruct((2, W), BF16)),
        in_specs=[VMEM, VMEM, VMEM, VMEM, pl.BlockSpec(memory_space=pltpu.SMEM), VMEM],
        out_specs=(VMEM, VMEM),
        compiler_params=pltpu.CompilerParams(vmem_limit_bytes=32 * 2**20),
        name="range_outputs",
    )(got, orders, row, col, hloc, heavy)


def body(measures, row_keys, orders, heavy_keys, key_slot):
    index_x, index_y = lax.axis_index("gx"), lax.axis_index("gy")
    device = index_x * GY + index_y
    rows = measures.shape[0]
    keys = row_keys.reshape(rows // LANES, LANES)
    pairs = jnp.repeat(heavy_keys.reshape(-1, 2), 2, axis=0)
    messages = gather(keys, measures, key_slot.reshape(KEYS // 256, 256), pairs)
    arrived = exchange(messages, "gx", GX, peer_gx, source_gx, 0)
    blocks = key_slot.reshape(GX, GY * KD)
    dense = owner(arrived, blocks)
    ring = functools.partial(peer_ring, GY), functools.partial(source_ring, GY)
    quarters = exchange(dense, "gy", GY, *ring, 1)
    own_blocks = lax.dynamic_slice_in_dim(blocks, index_y * KD, KD, axis=1)
    scaled, slot_rows, heavy = quarter(quarters, own_blocks)
    moved = exchange(scaled.reshape(GX, 8, W), "gx", GX, peer_gx, source_gx, 2)
    own_slots = lax.dynamic_slice_in_dim(key_slot, device * KD, KD)
    heavy_local = lax.dynamic_slice_in_dim(heavy_keys, device * 2, 2) - device * KD
    result, report = outputs(
        moved.reshape(KD, W), orders, own_slots.reshape(1, KD), own_slots.reshape(KD, 1),
        heavy_local, heavy,
    )
    return (result, report, slot_rows.reshape(KD))


def solution(mesh):
    return jax.shard_map(
        body,
        mesh=mesh,
        in_specs=(P(("gx", "gy"), None), P(("gx", "gy")), P(("gx", "gy"), None), P(), P()),
        out_specs=(P(("gx", "gy"), None), P(("gx", "gy"), None), P(("gx", "gy"))),
        check_vma=False,
    )
```

```python
import jax
import jax.numpy as jnp
from jax import lax
from jax.experimental import pallas as pl
from jax.experimental.pallas import tpu as pltpu
from jax.sharding import PartitionSpec as P

MESH = pl.DeviceIdType.MESH
F32, BF16, I32, I16 = jnp.float32, jnp.bfloat16, jnp.int32, jnp.int16
LN2 = 0.6931471805599453

W = 128
GX, GY = 64, 4
KEYS = 131072
KD = 512
OWN = 2048
CAPK = 64
HG = 8
MSG = 80
LANES = 1024
VMEM = pl.BlockSpec(memory_space=pltpu.VMEM)


def iota(shape, dim):
    return lax.broadcasted_iota(I32, shape, dim)


def onehot(rows, lanes, base, labels):
    labels = (labels - base).astype(I16)
    return jnp.where(iota((rows, lanes), 0).astype(I16) == labels, jnp.ones((), BF16), jnp.zeros((), BF16))


def dot(a, b):
    return jnp.dot(a, b, preferred_element_type=F32)


def dot_t(a, b):
    return lax.dot_general(a, b, (((1,), (1,)), ((), ())), preferred_element_type=F32)


def power(e):
    return jnp.exp(e * LN2)


def encode(v):
    top = jnp.max(jnp.abs(v), axis=1, keepdims=True)
    e = jnp.ceil(jnp.log(jnp.maximum(top, 1e-30)) * (1.0 / LN2) - 14.99)
    e = jnp.maximum(e, -100.0)
    q = jnp.floor(v * power(-e) + 0.5).astype(I32)
    return q, e


def slots_of(ks, me):
    mine = jnp.where((ks >> 11) == me, 1.0, 0.0)
    upper = jnp.where(iota((KD, KD), 0) < iota((KD, KD), 1), 1.0, 0.0).astype(BF16)
    w = dot(mine.astype(BF16), upper)
    pos = (ks & (KD - 1)).astype(F32)
    lane = iota((GX, W), 1)
    table = jnp.zeros((GX, W), F32)
    for k in range(8):
        s = jnp.sum(jnp.where((mine > 0.5) & (w == float(k)), pos, 0.0), axis=1, keepdims=True)
        table = jnp.where(lane == k, s, table)
    high = jnp.floor(table * (1.0 / 256.0))
    low = table - 256.0 * high
    repeat = jnp.where((iota((KD, GX), 0) >> 3) == iota((KD, GX), 1), 1.0, 0.0).astype(BF16)
    each = 256.0 * dot(repeat, high.astype(BF16)) + dot(repeat, low.astype(BF16))
    pick = iota((KD, W), 1) == (iota((KD, W), 0) & 7)
    return jnp.sum(jnp.where(pick, each, 0.0), axis=1, keepdims=True).astype(I32)


def offset(m):
    zi = 7 - m
    return ((zi + 1) // 2) * (1 - 2 * ((zi + 1) % 2))


def pair_at(me, dx, dz):
    z, x = (me // 2) % 8, me // 16
    return (((x + 4 + dx) % 4) * 8 + (z + 8 + dz) % 8) * 2


def join_kernel(keys_ref, x_ref, ks_ref, hk_ref, blocks_ref,
                moved_ref, slots_ref, heavy_ref,
                tab, shi_s, slo_s, seg_s, xe, pt, rk, acc, hq, hx, msg, arr,
                v_s, meta_s, scol, dense, tal, hsum, hcount, quarters, parts, scaled,
                ssem, rsem, ysend, yrecv, fsend, frecv):
    gx, gy = lax.axis_index("gx"), lax.axis_index("gy")
    barrier = pltpu.get_barrier_semaphore()

    def greet(k, carry):
        pl.semaphore_signal(barrier, inc=1, device_id={"gx": (gx + k) % GX}, device_id_type=MESH)
        return carry

    lax.fori_loop(1, GX, greet, 0)
    for k in range(1, GY):
        pl.semaphore_signal(barrier, inc=1, device_id={"gy": (gy + k) % GY}, device_id_type=MESH)

    chunks = keys_ref.shape[0]
    hi_n, lo_n = ks_ref.shape
    ks = ks_ref[...]
    key_id = iota((hi_n, lo_n), 0) * lo_n + iota((hi_n, lo_n), 1)
    p1 = (ks >> 11) * 2 + ((ks >> 8) & 1)
    p1 = jnp.where(key_id == hk_ref[:, 0:1], 128, p1)
    p1 = jnp.where(key_id == hk_ref[:, 1:2], 129, p1)
    tab[0:lo_n, :] = p1.astype(F32).T.astype(BF16)
    tab[lo_n : 2 * lo_n, :] = (ks & 255).astype(F32).T.astype(BF16)
    pt[...] = jnp.zeros_like(pt)

    def look(c, carry):
        key = keys_ref[pl.ds(c, 1), :]
        hi, lo = key >> 8, key & 255
        t = dot(tab[...], onehot(hi_n, LANES, 0, hi))
        mine = iota((lo_n, LANES), 0) == lo
        a = jnp.sum(jnp.where(mine, t[:lo_n], 0.0), axis=0, keepdims=True).astype(I32)
        b = jnp.sum(jnp.where(mine, t[lo_n:], 0.0), axis=0, keepdims=True).astype(I32)
        heavy = a >= 128
        shi = jnp.where(heavy, -1, (a >> 1) * 8 + ((key >> 9) & 3) * 2 + (a & 1))
        shi_s[pl.ds(c, 1), :] = shi
        slo_s[pl.ds(c, 1), :] = b
        seg_s[pl.ds(c, 1), :] = jnp.where(
            heavy, GX * CAPK + (key >> 9) * 2 + (a - 128), (a >> 1) * CAPK
        )
        pt[...] += dot_t(onehot(lo_n, LANES, 0, b), onehot(hi_n, LANES, 0, shi))
        return carry

    lax.fori_loop(0, chunks, look, 0, unroll=2)

    here = jnp.where(pt[...] > 0.5, 1.0, 0.0).astype(BF16)
    lower = jnp.where(iota((lo_n, lo_n), 1) < iota((lo_n, lo_n), 0), 1.0, 0.0).astype(BF16)
    r0, r1 = iota((hi_n, hi_n), 0), iota((hi_n, hi_n), 1)
    before = jnp.where((r0 < r1) & ((r0 >> 3) == (r1 >> 3)), 1.0, 0.0).astype(BF16)
    column = dot(jnp.ones((lo_n, lo_n), BF16), here).astype(BF16)
    rk[...] = (dot(lower, here) + dot(column, before)).astype(BF16)

    def rank(c, carry):
        shi = shi_s[pl.ds(c, 1), :]
        slo = slo_s[pl.ds(c, 1), :]
        t = dot(rk[...], onehot(hi_n, LANES, 0, shi))
        mine = iota((lo_n, LANES), 0) == slo
        r = jnp.sum(jnp.where(mine, t, 0.0), axis=0, keepdims=True).astype(I32)
        seg_s[pl.ds(c, 1), :] = seg_s[pl.ds(c, 1), :] + jnp.where(shi < 0, 0, r)
        line = iota((W, LANES), 0)
        ext = jnp.where(line == 0, 1, jnp.where(line == 1, slo, jnp.where(line == 2, shi & 7, 0)))
        at = pl.ds(pl.multiple_of(c * LANES, LANES), LANES)
        xe[at, 0:W] = x_ref[at, :]
        xe[at, W : 2 * W] = ext.astype(F32).T.astype(BF16)
        return carry

    lax.fori_loop(0, chunks, rank, 0, unroll=2)

    half = chunks // 2

    def sums(bases, c):
        total = None
        for i in range(half):
            at = pl.ds(pl.multiple_of((c * half + i) * LANES, LANES), LANES)
            seg = seg_s[pl.ds(c * half + i, 1), :]
            oh = jnp.concatenate([onehot(W, LANES, b, seg) for b in bases], axis=0)
            part = dot(oh, xe[at, :])
            total = part if total is None else total + part
        return total

    lane = iota((512, W), 1)
    first = [GX * CAPK + i * W for i in range(4)]
    acc[...] = sums(first, 0)
    acc[...] += sums(first, 1)
    q, e = encode(acc[:, 0:W])
    hq[...] = q
    hx[...] = jnp.where(lane == 64, acc[:, W : W + 1], jnp.where(lane == 65, e, 0.0)).astype(I32)
    pl.semaphore_wait(barrier, GX + GY - 2)

    def to_owner(o):
        return pltpu.make_async_remote_copy(
            src_ref=msg.at[o], dst_ref=arr.at[gx], send_sem=ssem.at[o], recv_sem=rsem.at[gx],
            device_id={"gx": o}, device_id_type=MESH,
        )

    def send(m):
        def one(i, carry):
            o = pair_at(gx, i // 2, offset(m)) + i % 2

            @pl.when(o != gx)
            def _():
                to_owner(o).start()

            return carry

        lax.fori_loop(0, 8, one, 0)

    def owners(m, carry):
        pairs = [pair_at(gx, dx, offset(m)) for dx in range(4)]
        bases = [p * CAPK for p in pairs]
        acc[...] = sums(bases, 0)

        @pl.when(m > 0)
        def _():
            send(m - 1)

        acc[...] += sums(bases, 1)
        q, e = encode(acc[:, 0:W])
        t = jnp.where(lane == 3, e, acc[:, W : 2 * W]).T[0:8]
        cnt = t[0:1]
        slot = jnp.where(
            cnt > 0.5, jnp.floor((t[1:2] + 256.0 * t[2:3]) / jnp.maximum(cnt, 1.0) + 0.5), -1.0
        )
        line = iota((8, 512), 0)
        meta = jnp.where(line == 0, slot, jnp.where(line == 1, cnt, t[3:4])).astype(I32)
        for i in range(8):
            o = pairs[i // 2] + i % 2
            part = meta[:, (i // 2) * W : (i // 2 + 1) * W]
            if i % 2:
                part = pltpu.roll(part, 64, 1)
            at = pl.ds(pl.multiple_of(o * 8, 8), 8)
            part = jnp.where(iota((8, W), 1) < 64, part, hx[at, :])
            values = q[i * 64 : (i + 1) * 64].astype(I16)
            tail = jnp.concatenate([hq[at, :], part], axis=0).astype(I16)
            msg[pl.ds(o, 1), 0:64, :] = values[None]
            msg[pl.ds(o, 1), 64:80, :] = tail[None]

            @pl.when(o == gx)
            def _():
                arr[pl.ds(o, 1), 0:64, :] = values[None]
                arr[pl.ds(o, 1), 64:80, :] = tail[None]

        return carry

    lax.fori_loop(0, 8, owners, 0)

    for q in range(GY):
        at = slice(q * KD, (q + 1) * KD)
        scol[at, :] = slots_of(blocks_ref[:, at], gx) + q * KD
    send(7)

    dense[...] = jnp.zeros_like(dense)
    tal[...] = jnp.zeros_like(tal)
    hsum[...] = jnp.zeros_like(hsum)
    hcount[...] = jnp.zeros_like(hcount)
    lane8 = iota((8, W), 1)

    def arrive(m, carry):
        for dx in range(4):
            pair = pair_at(gx, -dx, -offset(m))
            metas = []
            for i in range(2):
                s = pair + i

                @pl.when(s != gx)
                def _():
                    pltpu.make_async_remote_copy(
                        src_ref=msg.at[s], dst_ref=arr.at[s], send_sem=ssem.at[s],
                        recv_sem=rsem.at[s], device_id={"gx": s}, device_id_type=MESH,
                    ).wait_recv()

                q = arr[pl.ds(s, 1), 0:64, :][0].astype(I32)
                high = q >> 8
                at = slice((dx * 2 + i) * 64, (dx * 2 + i + 1) * 64)
                v_s[at, 0:W] = high.astype(F32).astype(BF16)
                v_s[at, W : 2 * W] = (q - high * 256).astype(F32).astype(BF16)
                tail = arr[pl.ds(s, 1), 64:80, :][0].astype(I32)
                meta = tail[8:16]
                hsum[...] += tail[0:8].astype(F32) * power(meta[:, 65:66].astype(F32))
                hcount[...] += meta[:, 64:65].astype(F32) + jnp.zeros((8, W), F32)
                metas.append(meta)
            meta_s[:, dx * W : (dx + 1) * W] = jnp.where(
                lane8 < 64, metas[0], pltpu.roll(metas[1], 64, 1)
            )
        meta = meta_s[...]
        scale = power(meta[2:3].astype(F32))
        count = meta[1:2].astype(F32)

        def quarter(q, carry):
            at = pl.ds(pl.multiple_of(q * KD, KD), KD)
            mine = scol[at, :] == meta[0:1]
            dense[at, :] += dot(jnp.where(mine, scale, 0.0).astype(BF16), v_s[...])
            hits = jnp.where(mine, count, 0.0)
            tal[at, :] += (hits[:, 0:W] + hits[:, W : 2 * W]) + (
                hits[:, 2 * W : 3 * W] + hits[:, 3 * W : 4 * W]
            )
            return carry

        lax.fori_loop(0, GY, quarter, 0)
        return carry

    lax.fori_loop(0, 8, arrive, 0)

    line8 = iota((8, W), 0)
    for q in range(GY):
        rows = jnp.where(line8 == 0, hsum[2 * q : 2 * q + 1], 0.0)
        rows = jnp.where(line8 == 1, hsum[2 * q + 1 : 2 * q + 2], rows)
        rows = jnp.where(line8 == 2, hcount[2 * q : 2 * q + 1], rows)
        rows = jnp.where(line8 == 3, hcount[2 * q + 1 : 2 * q + 2], rows)
        quarters[q, KD + 8 : KD + 16, :] = rows

    def to_quarter(p):
        return pltpu.make_async_remote_copy(
            src_ref=quarters.at[p], dst_ref=parts.at[gy], send_sem=ysend.at[p],
            recv_sem=yrecv.at[gy], device_id={"gy": p}, device_id_type=MESH,
        )

    def leave(k, carry):
        p = (gy + k) % GY
        at = pl.ds(pl.multiple_of(p * KD, KD), KD)
        quarters[pl.ds(p, 1), 0:KD, :] = (dense[at, 0:W] * 256.0 + dense[at, W : 2 * W])[None]
        t = jnp.sum(tal[at, :].T, axis=0, keepdims=True)
        rows = jnp.zeros((8, W), F32)
        for i in range(4):
            rows = jnp.where(line8 == i, t[:, i * W : (i + 1) * W], rows)
        quarters[pl.ds(p, 1), KD : KD + 8, :] = rows[None]

        @pl.when(k > 1)
        def _():
            to_quarter((gy + k - 1) % GY).start()

        return carry

    lax.fori_loop(1, GY + 1, leave, 0)
    pos = slots_of(blocks_ref[:, pl.ds(pl.multiple_of(gy * KD, KD), KD)], gx)
    total = quarters[pl.ds(gy, 1), :, :][0]
    for k in range(1, GY):
        s = (gy + GY - k) % GY
        pltpu.make_async_remote_copy(
            src_ref=quarters.at[s], dst_ref=parts.at[s], send_sem=ysend.at[s],
            recv_sem=yrecv.at[s], device_id={"gy": s}, device_id_type=MESH,
        ).wait_recv()
        total = total + parts[pl.ds(s, 1), :, :][0]

    counts = total[KD : KD + 8]
    square = jnp.concatenate([counts, jnp.zeros((W - 8, W), F32)], axis=0).T
    col = jnp.concatenate([square[:, i : i + 1] for i in range(4)], axis=0)
    scaled[...] = (total[0:KD] * lax.rsqrt(1.0 + col)).reshape(GX, 8, W)

    def to_range(p):
        return pltpu.make_async_remote_copy(
            src_ref=scaled.at[p], dst_ref=moved_ref.at[gx], send_sem=fsend.at[p],
            recv_sem=frecv.at[gx], device_id={"gx": p}, device_id_type=MESH,
        )

    slots_ref[...] = jnp.sum(jnp.where(pos == iota((KD, KD), 1), col, 0.0), axis=0, keepdims=True)
    tail = total[KD + 8 : KD + 16]
    heavy_ref[...] = tail * lax.rsqrt(1.0 + pltpu.roll(tail, 6, 0))

    def range_out(k, carry):
        p = pair_at(gx, (k // 2) % 4, offset(k // 8)) + k % 2

        @pl.when(p != gx)
        def _():
            to_range(p).start()

        return carry

    lax.fori_loop(0, GX, range_out, 0)
    moved_ref[pl.ds(gx, 1), :, :] = scaled[pl.ds(gx, 1), :, :]

    def finish(k, carry):
        s = (gx + k) % GX
        to_owner(s).wait_send()
        to_range(s).wait_send()
        pltpu.make_async_remote_copy(
            src_ref=scaled.at[s], dst_ref=moved_ref.at[s], send_sem=fsend.at[s],
            recv_sem=frecv.at[s], device_id={"gx": s}, device_id_type=MESH,
        ).wait_recv()
        return carry

    lax.fori_loop(1, GX, finish, 0)
    for k in range(1, GY):
        to_quarter((gy + k) % GY).wait_send()


def join(keys, x, ks, hk, blocks):
    rows = x.shape[0]
    chunks = rows // LANES
    dma = pltpu.SemaphoreType.DMA
    return pl.pallas_call(
        join_kernel,
        out_shape=(
            jax.ShapeDtypeStruct((GX, 8, W), F32),
            jax.ShapeDtypeStruct((1, KD), F32),
            jax.ShapeDtypeStruct((8, W), F32),
        ),
        in_specs=[VMEM] * 5,
        out_specs=(VMEM,) * 3,
        scratch_shapes=[
            pltpu.VMEM((512, 512), BF16),
            pltpu.VMEM((chunks, LANES), I32),
            pltpu.VMEM((chunks, LANES), I32),
            pltpu.VMEM((chunks, LANES), I32),
            pltpu.VMEM((rows, 2 * W), BF16),
            pltpu.VMEM((256, 512), F32),
            pltpu.VMEM((256, 512), BF16),
            pltpu.VMEM((512, 2 * W), F32),
            pltpu.VMEM((512, W), I32),
            pltpu.VMEM((512, W), I32),
            pltpu.VMEM((GX, MSG, W), I16),
            pltpu.VMEM((GX, MSG, W), I16),
            pltpu.VMEM((512, 2 * W), BF16),
            pltpu.VMEM((8, 512), I32),
            pltpu.VMEM((OWN, 1), I32),
            pltpu.VMEM((OWN, 2 * W), F32),
            pltpu.VMEM((OWN, W), F32),
            pltpu.VMEM((8, W), F32),
            pltpu.VMEM((8, W), F32),
            pltpu.VMEM((GY, KD + 16, W), F32),
            pltpu.VMEM((GY, KD + 16, W), F32),
            pltpu.VMEM((GX, 8, W), F32),
            dma((GX,)), dma((GX,)), dma((GY,)), dma((GY,)), dma((GX,)), dma((GX,)),
        ],
        compiler_params=pltpu.CompilerParams(
            collective_id=0, has_side_effects=True, vmem_limit_bytes=56 * 2**20
        ),
        name="join_rows",
    )(keys, x, ks, hk, blocks)


def result_kernel(got_ref, orders_ref, row_ref, col_ref, hloc_ref, heavy_ref, out_ref, report_ref):
    own_row = row_ref[...] >> 11
    own_col = col_ref[...] >> 11
    j0, j1 = iota((KD, KD), 0), iota((KD, KD), 1)
    w = jnp.sum(jnp.where((own_row == own_col) & (j1 < j0), 1.0, 0.0), axis=1, keepdims=True)
    place = own_col * 8 + w.astype(I32)
    oh = jnp.where(place == j1, 1.0, 0.0).astype(BF16)
    got = got_ref[...]
    high = got.astype(BF16)
    low = (got - high.astype(F32)).astype(BF16)
    total = dot(oh, high) + dot(oh, low)
    orders = orders_ref[...].astype(F32)
    line = iota((KD, W), 0)
    reports = []
    for h in range(2):
        here = line == hloc_ref[h]
        total = jnp.where(here, heavy_ref[h : h + 1, :], total)
        mine = jnp.sum(jnp.where(here, orders, 0.0), axis=0, keepdims=True)
        reports.append(mine * heavy_ref[h : h + 1, :])
    out_ref[...] = (orders * total).astype(BF16)
    report_ref[...] = jnp.concatenate(reports, axis=0).astype(BF16)


def outputs(got, orders, row, col, hloc, heavy):
    return pl.pallas_call(
        result_kernel,
        out_shape=(jax.ShapeDtypeStruct((KD, W), BF16), jax.ShapeDtypeStruct((2, W), BF16)),
        in_specs=[VMEM, VMEM, VMEM, VMEM, pl.BlockSpec(memory_space=pltpu.SMEM), VMEM],
        out_specs=(VMEM, VMEM),
        compiler_params=pltpu.CompilerParams(vmem_limit_bytes=32 * 2**20),
        name="range_outputs",
    )(got, orders, row, col, hloc, heavy)


def body(measures, row_keys, orders, heavy_keys, key_slot):
    device = lax.axis_index("gx") * GY + lax.axis_index("gy")
    rows = measures.shape[0]
    keys = row_keys.reshape(rows // LANES, LANES)
    pairs = jnp.repeat(heavy_keys.reshape(-1, 2), 2, axis=0)
    blocks = key_slot.reshape(GX, GY * KD)
    moved, slot_rows, heavy = join(
        keys, measures, key_slot.reshape(KEYS // 256, 256), pairs, blocks
    )
    own_slots = lax.dynamic_slice_in_dim(key_slot, device * KD, KD)
    heavy_local = lax.dynamic_slice_in_dim(heavy_keys, device * 2, 2) - device * KD
    result, report = outputs(
        moved.reshape(KD, W), orders, own_slots.reshape(1, KD), own_slots.reshape(KD, 1),
        heavy_local, heavy,
    )
    return (result, report, slot_rows.reshape(KD))


def solution(mesh):
    return jax.shard_map(
        body,
        mesh=mesh,
        in_specs=(P(("gx", "gy"), None), P(("gx", "gy")), P(("gx", "gy"), None), P(), P()),
        out_specs=(P(("gx", "gy"), None), P(("gx", "gy"), None), P(("gx", "gy"))),
        check_vma=False,
    )
```

```python
import jax
import jax.numpy as jnp
from jax import lax
from jax.experimental import pallas as pl
from jax.experimental.pallas import tpu as pltpu
from jax.sharding import PartitionSpec as P

MESH = pl.DeviceIdType.MESH
F32, BF16, I32, I16 = jnp.float32, jnp.bfloat16, jnp.int32, jnp.int16
LN2 = 0.6931471805599453

W = 128
GX, GY = 64, 4
KEYS = 131072
KD = 512
OWN = 2048
CAPK = 64
HG = 8
MSG = 80
LANES = 1024
VMEM = pl.BlockSpec(memory_space=pltpu.VMEM)


def iota(shape, dim):
    return lax.broadcasted_iota(I32, shape, dim)


def onehot(rows, lanes, base, labels):
    labels = (labels - base).astype(I16)
    return jnp.where(iota((rows, lanes), 0).astype(I16) == labels, jnp.ones((), BF16), jnp.zeros((), BF16))


def dot(a, b):
    return jnp.dot(a, b, preferred_element_type=F32)


def dot_t(a, b):
    return lax.dot_general(a, b, (((1,), (1,)), ((), ())), preferred_element_type=F32)


def power(e):
    return jnp.exp(e * LN2)


def encode(v):
    top = jnp.max(jnp.abs(v), axis=1, keepdims=True)
    e = jnp.ceil(jnp.log(jnp.maximum(top, 1e-30)) * (1.0 / LN2) - 14.99)
    e = jnp.maximum(e, -100.0)
    q = jnp.floor(v * power(-e) + 0.5).astype(I32)
    return q, e


def quarter_of(ks_ref, q):
    rows = [ks_ref[pl.ds(q * 4 + i, GX, stride=16), :] for i in range(4)]
    return jnp.concatenate(rows, axis=1)


def slots_of(ks, me):
    mine = jnp.where((ks >> 11) == me, 1.0, 0.0)
    upper = jnp.where(iota((KD, KD), 0) < iota((KD, KD), 1), 1.0, 0.0).astype(BF16)
    w = dot(mine.astype(BF16), upper)
    pos = (ks & (KD - 1)).astype(F32)
    lane = iota((GX, W), 1)
    table = jnp.zeros((GX, W), F32)
    for k in range(8):
        s = jnp.sum(jnp.where((mine > 0.5) & (w == float(k)), pos, 0.0), axis=1, keepdims=True)
        table = jnp.where(lane == k, s, table)
    high = jnp.floor(table * (1.0 / 256.0))
    low = table - 256.0 * high
    repeat = jnp.where((iota((KD, GX), 0) >> 3) == iota((KD, GX), 1), 1.0, 0.0).astype(BF16)
    each = 256.0 * dot(repeat, high.astype(BF16)) + dot(repeat, low.astype(BF16))
    pick = iota((KD, W), 1) == (iota((KD, W), 0) & 7)
    return jnp.sum(jnp.where(pick, each, 0.0), axis=1, keepdims=True).astype(I32)


def offset(m):
    zi = 7 - m
    return ((zi + 1) // 2) * (1 - 2 * ((zi + 1) % 2))


def pair_at(me, dx, dz):
    z, x = (me // 2) % 8, me // 16
    return (((x + 4 + dx) % 4) * 8 + (z + 8 + dz) % 8) * 2


def join_kernel(keys_ref, x_ref, ks_ref, hk_ref, heavy_ref, orders_ref,
                out_ref, report_ref, slots_ref,
                tab, shi_s, slo_s, seg_s, xe, pt, rk, acc, hq, hx, msg, arr,
                v_s, meta_s, scol, dense, tal, hsum, hcount, quarters, parts, hquart, hparts,
                scaled, moved, place_s, ssem, rsem, ysend, yrecv, hsend, hrecv, fsend, frecv, xsem):
    gx, gy = lax.axis_index("gx"), lax.axis_index("gy")
    barrier = pltpu.get_barrier_semaphore()
    rows_in = pltpu.make_async_copy(x_ref, xe.at[:, 0:W], xsem)
    rows_in.start()

    def greet(k, carry):
        pl.semaphore_signal(barrier, inc=1, device_id={"gx": (gx + k) % GX}, device_id_type=MESH)
        return carry

    lax.fori_loop(1, GX, greet, 0)
    for k in range(1, GY):
        pl.semaphore_signal(barrier, inc=1, device_id={"gy": (gy + k) % GY}, device_id_type=MESH)

    chunks = xe.shape[0] // LANES
    hi_n, lo_n = 512, 256
    for i in range(2):
        ks = ks_ref[pl.ds(i, hi_n, stride=2), :]
        p1 = (ks >> 11) * 2 + ((ks >> 8) & 1)
        tab[i * W : (i + 1) * W, :] = p1.astype(F32).T.astype(BF16)
        tab[lo_n + i * W : lo_n + (i + 1) * W, :] = (ks & 255).astype(F32).T.astype(BF16)
    hk = jnp.concatenate([hk_ref[i : i + 1, :] for i in range(4)], axis=1)
    line = iota((16, hi_n), 0)
    digits = jnp.where(line == 0, hk & 255, jnp.where(line == 1, (hk >> 8) & 1, 0))
    digits = digits.astype(F32).astype(BF16)
    block = 2 * (iota((hi_n, hi_n), 1) >> 1)
    odd = (iota((1, hi_n), 1) & 1).astype(F32)
    marks = jnp.full((16, hi_n), -1.0, F32)
    for i in range(2):
        pick = jnp.where(iota((hi_n, hi_n), 0) == block + i, 1.0, 0.0).astype(BF16)
        found = dot(digits, pick)
        marks = jnp.where(line == i, jnp.where(found[1:2] == odd, found[0:1], -1.0), marks)
    tab[2 * lo_n : 2 * lo_n + 16, :] = marks.astype(BF16)
    z0, x0 = (gx // 2) % 8, gx // 16
    pt[...] = jnp.zeros_like(pt)

    def look(c, carry):
        block = keys_ref[pl.ds(pl.multiple_of(c * 8, 8), 8), :]
        key = jnp.concatenate([block[i : i + 1] for i in range(8)], axis=1)
        hi, lo = key >> 8, key & 255
        t = dot(tab[...], onehot(hi_n, LANES, 0, hi))
        mine = iota((lo_n, LANES), 0) == lo
        a = jnp.sum(jnp.where(mine, t[:lo_n], 0.0), axis=0, keepdims=True).astype(I32)
        b = jnp.sum(jnp.where(mine, t[lo_n : 2 * lo_n], 0.0), axis=0, keepdims=True).astype(I32)
        low = lo.astype(F32)
        second = t[2 * lo_n + 1 : 2 * lo_n + 2] == low
        heavy = (t[2 * lo_n : 2 * lo_n + 1] == low) | second
        owner = a >> 1
        dx = ((owner >> 4) + 4 - x0) & 3
        dz = (((owner >> 1) & 7) + 8 - z0) & 7
        zi = jnp.where(dz == 0, 0, jnp.where(dz <= 4, 2 * dz - 1, 16 - 2 * dz))
        place = (7 - zi) * 8 + dx * 2 + (owner & 1)
        shi = jnp.where(heavy, -1, owner * 8 + ((key >> 9) & 3) * 2 + (a & 1))
        shi_s[pl.ds(c, 1), :] = shi
        slo_s[pl.ds(c, 1), :] = b
        seg_s[pl.ds(c, 1), :] = jnp.where(
            heavy, GX * CAPK + (key >> 9) * 2 + jnp.where(second, 1, 0), place * CAPK
        )
        pt[...] += dot_t(onehot(lo_n, LANES, 0, b), onehot(hi_n, LANES, 0, shi))
        return carry

    lax.fori_loop(0, chunks, look, 0, unroll=2)

    here = jnp.where(pt[...] > 0.5, 1.0, 0.0).astype(BF16)
    lower = jnp.where(iota((lo_n, lo_n), 1) < iota((lo_n, lo_n), 0), 1.0, 0.0).astype(BF16)
    r0, r1 = iota((hi_n, hi_n), 0), iota((hi_n, hi_n), 1)
    before = jnp.where((r0 < r1) & ((r0 >> 3) == (r1 >> 3)), 1.0, 0.0).astype(BF16)
    column = dot(jnp.ones((lo_n, lo_n), BF16), here).astype(BF16)
    rk[...] = (dot(lower, here) + dot(column, before)).astype(BF16)

    def rank(c, carry):
        shi = shi_s[pl.ds(c, 1), :]
        slo = slo_s[pl.ds(c, 1), :]
        t = dot(rk[...], onehot(hi_n, LANES, 0, shi))
        mine = iota((lo_n, LANES), 0) == slo
        r = jnp.sum(jnp.where(mine, t, 0.0), axis=0, keepdims=True).astype(I32)
        seg_s[pl.ds(c, 1), :] = seg_s[pl.ds(c, 1), :] + jnp.where(shi < 0, 0, r)
        line = iota((W, LANES), 0)
        ext = jnp.where(line == 0, 1, jnp.where(line == 1, slo, jnp.where(line == 2, shi & 7, 0)))
        at = pl.ds(pl.multiple_of(c * LANES, LANES), LANES)
        xe[at, W : 2 * W] = ext.astype(F32).T.astype(BF16)
        return carry

    lax.fori_loop(0, chunks, rank, 0, unroll=2)

    half = chunks // 2

    def sums(base, c):
        total = None
        for i in range(half):
            at = pl.ds(pl.multiple_of((c * half + i) * LANES, LANES), LANES)
            part = dot(onehot(512, LANES, base, seg_s[pl.ds(c * half + i, 1), :]), xe[at, :])
            total = part if total is None else total + part
        return total

    rows_in.wait()
    lane = iota((512, W), 1)
    acc[...] = sums(GX * CAPK, 0) + sums(GX * CAPK, 1)
    q, e = encode(acc[:, 0:W])
    hq[...] = q
    hx[...] = jnp.where(lane == 64, acc[:, W : W + 1], jnp.where(lane == 65, e, 0.0)).astype(I32)
    pl.semaphore_wait(barrier, GX + GY - 2)

    def to_owner(o):
        return pltpu.make_async_remote_copy(
            src_ref=msg.at[o], dst_ref=arr.at[gx], send_sem=ssem.at[o], recv_sem=rsem.at[gx],
            device_id={"gx": o}, device_id_type=MESH,
        )

    def send(m):
        def one(i, carry):
            o = pair_at(gx, i // 2, offset(m)) + i % 2

            @pl.when(o != gx)
            def _():
                to_owner(o).start()

            return carry

        lax.fori_loop(0, 8, one, 0)

    def owners(m, carry):
        pairs = [pair_at(gx, dx, offset(m)) for dx in range(4)]

        def step(c, carry):
            @pl.when((c > 0) & (m > 0))
            def _():
                send(m - 1)

            acc[...] = jnp.where(c > 0, acc[...], 0.0) + sums(m * 512, c)
            return carry

        lax.fori_loop(0, 2, step, 0)
        q, e = encode(acc[:, 0:W])
        t = jnp.where(lane == 3, e, acc[:, W : 2 * W]).T[0:8]
        cnt = t[0:1]
        slot = jnp.where(
            cnt > 0.5, jnp.floor((t[1:2] + 256.0 * t[2:3]) / jnp.maximum(cnt, 1.0) + 0.5), -1.0
        )
        line = iota((8, 512), 0)
        meta = jnp.where(line == 0, slot, jnp.where(line == 1, cnt, t[3:4])).astype(I32)
        for i in range(8):
            o = pairs[i // 2] + i % 2
            part = meta[:, (i // 2) * W : (i // 2 + 1) * W]
            if i % 2:
                part = pltpu.roll(part, 64, 1)
            at = pl.ds(pl.multiple_of(o * 8, 8), 8)
            part = jnp.where(iota((8, W), 1) < 64, part, hx[at, :])
            values = q[i * 64 : (i + 1) * 64].astype(I16)
            tail = jnp.concatenate([hq[at, :], part], axis=0).astype(I16)
            msg[pl.ds(o, 1), 0:64, :] = values[None]
            msg[pl.ds(o, 1), 64:80, :] = tail[None]

            @pl.when(o == gx)
            def _():
                arr[pl.ds(o, 1), 0:64, :] = values[None]
                arr[pl.ds(o, 1), 64:80, :] = tail[None]

        return carry

    lax.fori_loop(0, 8, owners, 0)

    for q in range(GY):
        at = slice(q * KD, (q + 1) * KD)
        scol[at, :] = slots_of(quarter_of(ks_ref, q), gx) + q * KD
    send(7)

    dense[...] = jnp.zeros_like(dense)
    tal[...] = jnp.zeros_like(tal)
    hsum[...] = jnp.zeros_like(hsum)
    hcount[...] = jnp.zeros_like(hcount)
    lane8 = iota((8, W), 1)

    def arrive(m, carry):
        for dx in range(4):
            pair = pair_at(gx, -dx, -offset(m))
            metas = []
            for i in range(2):
                s = pair + i

                @pl.when(s != gx)
                def _():
                    pltpu.make_async_remote_copy(
                        src_ref=msg.at[s], dst_ref=arr.at[s], send_sem=ssem.at[s],
                        recv_sem=rsem.at[s], device_id={"gx": s}, device_id_type=MESH,
                    ).wait_recv()

                q = arr[pl.ds(s, 1), 0:64, :][0].astype(I32)
                high = q >> 8
                at = slice((dx * 2 + i) * 64, (dx * 2 + i + 1) * 64)
                v_s[at, 0:W] = high.astype(F32).astype(BF16)
                v_s[at, W : 2 * W] = (q - high * 256).astype(F32).astype(BF16)
                tail = arr[pl.ds(s, 1), 64:80, :][0].astype(I32)
                meta = tail[8:16]
                hsum[...] += tail[0:8].astype(F32) * power(meta[:, 65:66].astype(F32))
                hcount[...] += meta[:, 64:65].astype(F32) + jnp.zeros((8, W), F32)
                metas.append(meta)
            meta_s[:, dx * W : (dx + 1) * W] = jnp.where(
                lane8 < 64, metas[0], pltpu.roll(metas[1], 64, 1)
            )
        meta = meta_s[...]
        scale = power(meta[2:3].astype(F32))
        count = meta[1:2].astype(F32)

        for q in range(GY):
            at = slice(q * KD, (q + 1) * KD)
            mine = scol[at, :] == meta[0:1]
            dense[at, :] += dot(jnp.where(mine, scale, 0.0).astype(BF16), v_s[...])
            hits = jnp.where(mine, count, 0.0)
            tal[at, :] += (hits[:, 0:W] + hits[:, W : 2 * W]) + (
                hits[:, 2 * W : 3 * W] + hits[:, 3 * W : 4 * W]
            )
        return carry

    lax.fori_loop(0, 8, arrive, 0)

    line8 = iota((8, W), 0)
    for q in range(GY):
        rows = jnp.where(line8 == 0, hsum[2 * q : 2 * q + 1], 0.0)
        rows = jnp.where(line8 == 1, hsum[2 * q + 1 : 2 * q + 2], rows)
        rows = jnp.where(line8 == 2, hcount[2 * q : 2 * q + 1], rows)
        rows = jnp.where(line8 == 3, hcount[2 * q + 1 : 2 * q + 2], rows)
        hquart[q, :, :] = rows

    def to_quarter(p):
        return pltpu.make_async_remote_copy(
            src_ref=quarters.at[p], dst_ref=parts.at[gy], send_sem=ysend.at[p],
            recv_sem=yrecv.at[gy], device_id={"gy": p}, device_id_type=MESH,
        )

    def heavy_to(p):
        return pltpu.make_async_remote_copy(
            src_ref=hquart.at[p], dst_ref=hparts.at[gy], send_sem=hsend.at[p],
            recv_sem=hrecv.at[gy], device_id={"gy": p}, device_id_type=MESH,
        )

    def leave(k, carry):
        p = (gy + k) % GY
        at = pl.ds(pl.multiple_of(p * KD, KD), KD)
        q, e = encode(dense[at, 0:W] * 256.0 + dense[at, W : 2 * W])
        q = q.astype(I16)
        t = jnp.sum(tal[at, :].T, axis=0, keepdims=True)
        e = jnp.where(lane == 0, e, 0.0).T[0:1]
        line = iota((16, W), 0)
        rows = jnp.zeros((16, W), F32)
        for i in range(4):
            rows = jnp.where(line == i, t[:, i * W : (i + 1) * W], rows)
            rows = jnp.where(line == 4 + i, e[:, i * W : (i + 1) * W], rows)
        rows = rows.astype(I32).astype(I16)
        quarters[pl.ds(p, 1), 0:KD, :] = q[None]
        quarters[pl.ds(p, 1), KD : KD + 16, :] = rows[None]

        @pl.when(k > 1)
        def _():
            to_quarter((gy + k - 1) % GY).start()

        @pl.when(k == GY)
        def _():
            parts[pl.ds(gy, 1), 0:KD, :] = q[None]
            parts[pl.ds(gy, 1), KD : KD + 16, :] = rows[None]

        return carry

    lax.fori_loop(1, GY + 1, leave, 0)
    for k in range(1, GY):
        heavy_to((gy + k) % GY).start()
    pos = slots_of(quarter_of(ks_ref, gy), gx)

    device = gx * GY + gy
    owners_here = [ks_ref[pl.ds(device * 4 + i, 1), :] >> 11 for i in range(4)]
    row = jnp.concatenate(owners_here, axis=1)
    square = jnp.zeros((W, W), I32)
    for i in range(4):
        square = jnp.where(iota((W, W), 0) == i, owners_here[i], square)
    square = square.astype(F32).T.astype(I32)
    col = jnp.concatenate([square[:, i : i + 1] for i in range(4)], axis=0)
    j0, j1 = iota((KD, KD), 0), iota((KD, KD), 1)
    w = jnp.sum(jnp.where((row == col) & (j1 < j0), 1.0, 0.0), axis=1, keepdims=True)
    place_s[...] = jnp.where(col * 8 + w.astype(I32) == j1, 1.0, 0.0).astype(BF16)

    total, tallies = jnp.zeros((KD, W), F32), jnp.zeros((W, W), F32)
    tail = hquart[pl.ds(gy, 1), :, :][0]
    for k in range(GY):
        s = (gy + GY - k) % GY
        if k:
            for sent, got, ss, rs in ((quarters, parts, ysend, yrecv), (hquart, hparts, hsend, hrecv)):
                pltpu.make_async_remote_copy(
                    src_ref=sent.at[s], dst_ref=got.at[s], send_sem=ss.at[s], recv_sem=rs.at[s],
                    device_id={"gy": s}, device_id_type=MESH,
                ).wait_recv()
            tail = tail + hparts[pl.ds(s, 1), :, :][0]
        rows = parts[pl.ds(s, 1), KD : KD + 16, :][0].astype(F32)
        square = jnp.concatenate([rows, jnp.zeros((W - 16, W), F32)], axis=0).T
        scale = jnp.concatenate([square[:, 4 + i : 5 + i] for i in range(4)], axis=0)
        total = total + parts[pl.ds(s, 1), 0:KD, :][0].astype(F32) * power(scale)
        tallies = tallies + square

    col = jnp.concatenate([tallies[:, i : i + 1] for i in range(4)], axis=0)
    scaled[...] = (total * lax.rsqrt(1.0 + col)).reshape(GX, 8, W)

    def to_range(p):
        return pltpu.make_async_remote_copy(
            src_ref=scaled.at[p], dst_ref=moved.at[gx], send_sem=fsend.at[p],
            recv_sem=frecv.at[gx], device_id={"gx": p}, device_id_type=MESH,
        )

    slots = jnp.sum(jnp.where(pos == j1, col, 0.0), axis=0, keepdims=True)
    slots_ref[...] = jnp.concatenate([slots[:, i * W : (i + 1) * W] for i in range(4)], axis=0)

    def range_out(k, carry):
        p = pair_at(gx, (k // 2) % 4, offset(k // 8)) + k % 2

        @pl.when(p != gx)
        def _():
            to_range(p).start()

        return carry

    lax.fori_loop(0, GX, range_out, 0)
    moved[pl.ds(gx, 1), :, :] = scaled[pl.ds(gx, 1), :, :]

    def finish(k, carry):
        s = (gx + k) % GX
        to_owner(s).wait_send()
        to_range(s).wait_send()
        pltpu.make_async_remote_copy(
            src_ref=scaled.at[s], dst_ref=moved.at[s], send_sem=fsend.at[s],
            recv_sem=frecv.at[s], device_id={"gx": s}, device_id_type=MESH,
        ).wait_recv()
        return carry

    lax.fori_loop(1, GX, finish, 0)
    for k in range(1, GY):
        to_quarter((gy + k) % GY).wait_send()
        heavy_to((gy + k) % GY).wait_send()

    got = moved[...].reshape(KD, W)
    high = got.astype(BF16)
    low = (got - high.astype(F32)).astype(BF16)
    both = dot(place_s[...], jnp.concatenate([high, low], axis=1))
    total = both[:, 0:W] + both[:, W : 2 * W]
    orders = orders_ref[...].astype(F32)
    heavy = tail * lax.rsqrt(1.0 + pltpu.roll(tail, 6, 0))
    line = iota((KD, W), 0)
    reports = []
    for h in range(2):
        here = line == heavy_ref[2 * device + h] - device * KD
        total = jnp.where(here, heavy[h : h + 1, :], total)
        mine = jnp.sum(jnp.where(here, orders, 0.0), axis=0, keepdims=True)
        reports.append(mine * heavy[h : h + 1, :])
    out_ref[...] = (orders * total).astype(BF16)
    report_ref[...] = jnp.concatenate(reports, axis=0).astype(BF16)


def join(keys, x, ks, heavy_keys, orders):
    rows = x.shape[0]
    chunks = rows // LANES
    dma = pltpu.SemaphoreType.DMA
    return pl.pallas_call(
        join_kernel,
        out_shape=(
            jax.ShapeDtypeStruct((KD, W), BF16),
            jax.ShapeDtypeStruct((2, W), BF16),
            jax.ShapeDtypeStruct((4, W), F32),
        ),
        in_specs=[
            VMEM, pl.BlockSpec(memory_space=pl.ANY), VMEM, VMEM,
            pl.BlockSpec(memory_space=pltpu.SMEM), VMEM,
        ],
        out_specs=(VMEM,) * 3,
        scratch_shapes=[
            pltpu.VMEM((528, 512), BF16),
            pltpu.VMEM((chunks, LANES), I32),
            pltpu.VMEM((chunks, LANES), I32),
            pltpu.VMEM((chunks, LANES), I32),
            pltpu.VMEM((rows, 2 * W), BF16),
            pltpu.VMEM((256, 512), F32),
            pltpu.VMEM((256, 512), BF16),
            pltpu.VMEM((512, 2 * W), F32),
            pltpu.VMEM((512, W), I32),
            pltpu.VMEM((512, W), I32),
            pltpu.VMEM((GX, MSG, W), I16),
            pltpu.VMEM((GX, MSG, W), I16),
            pltpu.VMEM((512, 2 * W), BF16),
            pltpu.VMEM((8, 512), I32),
            pltpu.VMEM((OWN, 1), I32),
            pltpu.VMEM((OWN, 2 * W), F32),
            pltpu.VMEM((OWN, W), F32),
            pltpu.VMEM((8, W), F32),
            pltpu.VMEM((8, W), F32),
            pltpu.VMEM((GY, KD + 16, W), I16),
            pltpu.VMEM((GY, KD + 16, W), I16),
            pltpu.VMEM((GY, 8, W), F32),
            pltpu.VMEM((GY, 8, W), F32),
            pltpu.VMEM((GX, 8, W), F32),
            pltpu.VMEM((GX, 8, W), F32),
            pltpu.VMEM((KD, KD), BF16),
            dma((GX,)), dma((GX,)), dma((GY,)), dma((GY,)), dma((GY,)), dma((GY,)),
            dma((GX,)), dma((GX,)), dma,
        ],
        compiler_params=pltpu.CompilerParams(
            collective_id=0, has_side_effects=True, vmem_limit_bytes=56 * 2**20
        ),
        name="join_rows",
    )(keys, x, ks, heavy_keys.reshape(-1, W), heavy_keys, orders)


def hand_on_kernel(a_ref, b_ref, c_ref, out_a, out_b, out_c):
    out_a[...] = a_ref[...]
    out_b[...] = b_ref[...]
    out_c[...] = c_ref[...]


def hand_on(*arrays):
    return pl.pallas_call(
        hand_on_kernel,
        out_shape=tuple(jax.ShapeDtypeStruct(a.shape, a.dtype) for a in arrays),
        in_specs=[VMEM] * 3,
        out_specs=(VMEM,) * 3,
        name="hand_on",
    )(*arrays)


def body(measures, row_keys, orders, heavy_keys, key_slot):
    result, report, slot_rows = join(
        row_keys.reshape(-1, W), measures, key_slot.reshape(-1, W), heavy_keys, orders
    )
    result, report, slot_rows = hand_on(result, report, slot_rows)
    return (result, report, slot_rows.reshape(KD))


def solution(mesh):
    return jax.shard_map(
        body,
        mesh=mesh,
        in_specs=(P(("gx", "gy"), None), P(("gx", "gy")), P(("gx", "gy"), None), P(), P()),
        out_specs=(P(("gx", "gy"), None), P(("gx", "gy"), None), P(("gx", "gy"))),
        check_vma=False,
    )
```

```python
import jax
import jax.numpy as jnp
from jax import lax
from jax.experimental import pallas as pl
from jax.experimental.pallas import tpu as pltpu
from jax.sharding import PartitionSpec as P

MESH = pl.DeviceIdType.MESH
F32, BF16, I32, I16 = jnp.float32, jnp.bfloat16, jnp.int32, jnp.int16
LN2 = 0.6931471805599453

W = 128
GX, GY = 64, 4
KEYS = 131072
KD = 512
HK = 256
OWN = 2048
CAPK = 64
HALF = 2048
HG = 8
MSG = 80
LANES = 1024
VMEM = pl.BlockSpec(memory_space=pltpu.VMEM)


def iota(shape, dim):
    return lax.broadcasted_iota(I32, shape, dim)


def onehot(rows, lanes, base, labels):
    labels = (labels - base).astype(I16)
    return jnp.where(iota((rows, lanes), 0).astype(I16) == labels, jnp.ones((), BF16), jnp.zeros((), BF16))


def dot(a, b):
    return jnp.dot(a, b, preferred_element_type=F32)


def dot_t(a, b):
    return lax.dot_general(a, b, (((1,), (1,)), ((), ())), preferred_element_type=F32)


def power(e):
    return jnp.exp(e * LN2)


def encode(v):
    top = jnp.max(jnp.abs(v), axis=1, keepdims=True)
    e = jnp.ceil(jnp.log(jnp.maximum(top, 1e-30)) * (1.0 / LN2) - 14.99)
    e = jnp.maximum(e, -100.0)
    q = jnp.floor(v * power(-e) + 0.5).astype(I32)
    return q, e


def quarter_of(ks_ref, q):
    rows = [ks_ref[pl.ds(q * 4 + i, GX, stride=16), :] for i in range(4)]
    return jnp.concatenate(rows, axis=1)


def slots_of(ks, me):
    mine = jnp.where((ks >> 11) == me, 1.0, 0.0)
    upper = jnp.where(iota((KD, KD), 0) < iota((KD, KD), 1), 1.0, 0.0).astype(BF16)
    w = dot(mine.astype(BF16), upper)
    pos = (ks & (KD - 1)).astype(F32)
    lane = iota((GX, W), 1)
    table = jnp.zeros((GX, W), F32)
    for k in range(8):
        s = jnp.sum(jnp.where((mine > 0.5) & (w == float(k)), pos, 0.0), axis=1, keepdims=True)
        table = jnp.where(lane == k, s, table)
    high = jnp.floor(table * (1.0 / 256.0))
    low = table - 256.0 * high
    place = iota((KD, GX), 0) >> 3
    zi = 7 - (place >> 3)
    dz = ((zi + 1) >> 1) * (1 - 2 * ((zi + 1) & 1))
    z, x = (me // 2) % 8 + 8 + dz, me // 16 + ((place >> 1) & 3)
    block = ((x & 3) * 8 + (z & 7)) * 2 + (place & 1)
    repeat = jnp.where(block == iota((KD, GX), 1), 1.0, 0.0).astype(BF16)
    each = 256.0 * dot(repeat, high.astype(BF16)) + dot(repeat, low.astype(BF16))
    pick = iota((KD, W), 1) == (iota((KD, W), 0) & 7)
    return jnp.sum(jnp.where(pick, each, 0.0), axis=1, keepdims=True).astype(I32)


def offset(m):
    zi = 7 - m
    return ((zi + 1) // 2) * (1 - 2 * ((zi + 1) % 2))


def pair_at(me, dx, dz):
    z, x = (me // 2) % 8, me // 16
    return (((x + 4 + dx) % 4) * 8 + (z + 8 + dz) % 8) * 2


def join_kernel(keys_in, x_in, ks_in, hk_in, orders_in,
                out_ref, report_ref, slots_ref,
                keys_ref, ks_ref, hk_ref, orders_ref, tab, shi_s, slo_s, seg_s, run_s, xin, xm, xe, pt, rk, acc, ext, cnt_s, slot_s,
                hq, hx, msg, arr,
                v_s, meta_s, scol, dense, tal, hsum, hcount, quarters, parts, hquart, hparts,
                scaled, moved, place_s, poscol, slots_s, ssem, rsem, ysend, yrecv, hsend, hrecv, fsend, frecv, isem):
    gx, gy = lax.axis_index("gx"), lax.axis_index("gy")
    barrier = pltpu.get_barrier_semaphore()
    pairs = ((ks_in, ks_ref), (hk_in, hk_ref), (keys_in, keys_ref), (x_in, xin), (orders_in, orders_ref))
    inputs = [pltpu.make_async_copy(a, b, isem.at[i]) for i, (a, b) in enumerate(pairs)]
    for copy in inputs:
        copy.start()

    def greet(m, carry):
        for i in range(8):
            p = pair_at(gx, i // 2, offset(m)) + i % 2

            @pl.when(p != gx)
            def _():
                pl.semaphore_signal(barrier, inc=1, device_id={"gx": p}, device_id_type=MESH)

        return carry

    lax.fori_loop(0, 8, greet, 0)
    for k in range(1, GY):
        pl.semaphore_signal(barrier, inc=1, device_id={"gy": (gy + k) % GY}, device_id_type=MESH)

    chunks = xe.shape[0] // LANES
    hi_n, lo_n = 512, 256
    inputs[0].wait()
    inputs[1].wait()
    for i in range(2):
        ks = ks_ref[pl.ds(i, hi_n, stride=2), :]
        p1 = (ks >> 11) * 2 + ((ks >> 8) & 1)
        tab[i * W : (i + 1) * W, :] = p1.astype(F32).T.astype(BF16)
        tab[lo_n + i * W : lo_n + (i + 1) * W, :] = (ks & 255).astype(F32).T.astype(BF16)
    hk = jnp.concatenate([hk_ref[i : i + 1, :] for i in range(4)], axis=1)
    line = iota((16, hi_n), 0)
    digits = jnp.where(line == 0, hk & 255, jnp.where(line == 1, (hk >> 8) & 1, 0))
    digits = digits.astype(F32).astype(BF16)
    block = 2 * (iota((hi_n, hi_n), 1) >> 1)
    odd = (iota((1, hi_n), 1) & 1).astype(F32)
    marks = jnp.full((16, hi_n), -1.0, F32)
    for i in range(2):
        pick = jnp.where(iota((hi_n, hi_n), 0) == block + i, 1.0, 0.0).astype(BF16)
        found = dot(digits, pick)
        marks = jnp.where(line == i, jnp.where(found[1:2] == odd, found[0:1], -1.0), marks)
    tab[2 * lo_n : 2 * lo_n + 16, :] = marks.astype(BF16)
    z0, x0 = (gx // 2) % 8, gx // 16
    pt[...] = jnp.zeros_like(pt)

    def look(c, carry):
        block = keys_ref[pl.ds(pl.multiple_of(c * 8, 8), 8), :]
        key = jnp.concatenate([block[i : i + 1] for i in range(8)], axis=1)
        hi, lo = key >> 8, key & 255
        t = dot(tab[...], onehot(hi_n, LANES, 0, hi))
        mine = iota((lo_n, LANES), 0) == lo
        a = jnp.sum(jnp.where(mine, t[:lo_n], 0.0), axis=0, keepdims=True).astype(I32)
        b = jnp.sum(jnp.where(mine, t[lo_n : 2 * lo_n], 0.0), axis=0, keepdims=True).astype(I32)
        low = lo.astype(F32)
        second = t[2 * lo_n + 1 : 2 * lo_n + 2] == low
        heavy = (t[2 * lo_n : 2 * lo_n + 1] == low) | second
        owner = a >> 1
        dx = ((owner >> 4) + 4 - x0) & 3
        dz = (((owner >> 1) & 7) + 8 - z0) & 7
        zi = jnp.where(dz == 0, 0, jnp.where(dz <= 4, 2 * dz - 1, 16 - 2 * dz))
        place = (7 - zi) * 8 + dx * 2 + (owner & 1)
        shi = jnp.where(heavy, -1, owner * 8 + ((key >> 9) & 3) * 2 + (a & 1))
        shi_s[pl.ds(c, 1), :] = shi
        slo_s[pl.ds(c, 1), :] = b
        hid = (key >> 9) * 2 + jnp.where(second, 1, 0)
        seg_s[pl.ds(c, 1), :] = jnp.where(heavy, HALF + (hid & 255), (place >> 1) * CAPK)
        run_s[pl.ds(c, 1), :] = jnp.where(heavy, 2 * GX + (hid >> 5), (place >> 5) * CAPK)
        sub = jnp.where(heavy, hid, place) & 31
        line = iota((W, LANES), 0)
        kind = line >> 5
        facts = jnp.where(kind == 0, 1, jnp.where(kind == 1, b, jnp.where(kind == 2, shi & 7, 0)))
        facts = jnp.where((line & 31) == sub, facts, 0)
        at = pl.ds(pl.multiple_of(c * LANES, LANES), LANES)
        xm[at, :] = facts.astype(F32).T.astype(BF16)
        side = jnp.where(heavy, hid >> 8, place & 1).astype(F32)
        sides = jnp.broadcast_to(side, (W, LANES)).T.astype(BF16)
        x = xin[at, :]
        right = x * sides
        xe[at, 0:W] = x - right
        xe[at, W : 2 * W] = right
        pt[...] += dot_t(onehot(hi_n, LANES, 0, shi), onehot(lo_n, LANES, 0, b))
        return carry

    inputs[2].wait()
    inputs[3].wait()
    lax.fori_loop(0, chunks, look, 0, unroll=2)

    here = jnp.where(pt[...] > 0.5, 1.0, 0.0).T.astype(BF16)
    lower = jnp.where(iota((lo_n, lo_n), 1) < iota((lo_n, lo_n), 0), 1.0, 0.0).astype(BF16)
    r0, r1 = iota((hi_n, hi_n), 0), iota((hi_n, hi_n), 1)
    before = jnp.where((r0 < r1) & ((r0 >> 3) == (r1 >> 3)), 1.0, 0.0).astype(BF16)
    column = dot(jnp.ones((lo_n, lo_n), BF16), here).astype(BF16)
    rk[...] = (dot(lower, here) + dot(column, before)).astype(BF16)

    def rank(c, carry):
        shi = shi_s[pl.ds(c, 1), :]
        slo = slo_s[pl.ds(c, 1), :]
        t = dot(rk[...], onehot(hi_n, LANES, 0, shi))
        mine = iota((lo_n, LANES), 0) == slo
        r = jnp.sum(jnp.where(mine, t, 0.0), axis=0, keepdims=True).astype(I32)
        r = jnp.where(shi < 0, 0, r)
        seg_s[pl.ds(c, 1), :] = seg_s[pl.ds(c, 1), :] + r
        run_s[pl.ds(c, 1), :] = run_s[pl.ds(c, 1), :] + r
        return carry

    lax.fori_loop(0, chunks, rank, 0, unroll=2)

    def sums(base):
        total = None
        for c in range(chunks):
            at = slice(c * LANES, (c + 1) * LANES)
            part = dot(onehot(256, LANES, base, seg_s[c : c + 1, :]), xe[at, :])
            total = part if total is None else total + part
        return total

    ext[...] = jnp.zeros_like(ext)

    def gather_facts(c, carry):
        at = pl.ds(pl.multiple_of(c * LANES, LANES), LANES)
        ext[...] += dot(onehot(2 * GX + 16, LANES, 0, run_s[pl.ds(c, 1), :]), xm[at, :])
        return carry

    lax.fori_loop(0, chunks, gather_facts, 0, unroll=4)
    square = ext[0 : 2 * GX, :].T
    cnt = square[0:32]
    slot = jnp.floor((square[32:64] + 256.0 * square[64:96]) / jnp.maximum(cnt, 1.0) + 0.5)
    slot = jnp.where(cnt > 0.5, slot, -1.0)
    cnt_s[0:32, :] = cnt.astype(I32)
    cnt_s[32:64, :] = pltpu.roll(cnt, 64, 1).astype(I32)
    slot_s[0:32, :] = slot.astype(I32)
    slot_s[32:64, :] = pltpu.roll(slot, 64, 1).astype(I32)

    lane = iota((512, W), 1)
    counts = ext[2 * GX : 2 * GX + 16, :]
    high = jnp.floor(counts * (1.0 / 256.0))
    spread = jnp.where((iota((512, 16), 0) >> 5) == iota((512, 16), 1), 1.0, 0.0).astype(BF16)
    each = 256.0 * dot(spread, high.astype(BF16)) + dot(spread, (counts - 256.0 * high).astype(BF16))
    pick = lane == (iota((512, W), 0) & 31)
    counts = jnp.sum(jnp.where(pick, each, 0.0), axis=1, keepdims=True)

    def pack_heavy():
        both = acc[0]
        q, e = encode(jnp.concatenate([both[:, 0:W], both[:, W : 2 * W]], axis=0))
        hq[...] = q
        hx[...] = jnp.where(lane == 64, counts, jnp.where(lane == 65, e, 0.0)).astype(I32)

    acc[...] = jnp.zeros_like(acc)
    hq[...] = jnp.zeros_like(hq)
    hx[...] = jnp.zeros_like(hx)
    pl.semaphore_wait(barrier, GX + GY - 2)

    def to_owner(o):
        return pltpu.make_async_remote_copy(
            src_ref=msg.at[o], dst_ref=arr.at[gx], send_sem=ssem.at[o], recv_sem=rsem.at[gx],
            device_id={"gx": o}, device_id_type=MESH,
        )

    def send(m):
        for i in range(8):
            o = pair_at(gx, i // 2, offset(m)) + i % 2

            @pl.when(o != gx)
            def _():
                to_owner(o).start()

    def pack(m, both):
        q0, e0 = encode(both[:, 0:W])
        q1, e1 = encode(both[:, W : 2 * W])
        lane = iota((256, W), 1)
        e = jnp.where(lane == 0, e0, jnp.where(lane == 1, e1, 0.0)).T[0:8].astype(I32)
        pairs = [pair_at(gx, dx, offset(m)) for dx in range(4)]
        at = pl.ds(pl.multiple_of(m * 8, 8), 8)
        slots, counts = slot_s[at, :], cnt_s[at, :]
        lane, line = iota((8, W), 1), iota((8, W), 0)
        for i in range(8):
            o = pairs[i // 2] + i % 2
            part = e[i % 2 : i % 2 + 1, (i // 4) * W : (i // 4 + 1) * W]
            exps = pltpu.roll(part, 64, 1) if (i // 2) % 2 else part
            meta = jnp.where(line == 0, slots[i : i + 1], jnp.where(line == 1, counts[i : i + 1], exps))
            at = pl.ds(pl.multiple_of(o * 8, 8), 8)
            meta = jnp.where(lane < 64, meta, hx[at, :])
            values = (q1 if i % 2 else q0)[(i // 2) * 64 : (i // 2 + 1) * 64]
            msg[pl.ds(o, 1), 0:64, :] = values.astype(I16)[None]
            tail = jnp.concatenate([hq[at, :], meta], axis=0).astype(I16)
            msg[pl.ds(o, 1), 64:80, :] = tail[None]

    def owners(t, carry):
        @pl.when(t == 1)
        def _():
            pack_heavy()

        @pl.when(t == 2)
        def _():
            pack(0, acc[1])
            scol[0:KD, :] = slots_of(quarter_of(ks_ref, 0), gx)
            send(0)

        @pl.when(t > 3)
        def _():
            send(t - 3)

        pack(jnp.maximum(t - 2, 1), acc[pl.ds((t + 1) % 2, 1), :, :][0])
        acc[pl.ds(t % 2, 1), :, :] = sums(((t + 8) % 9) * 256)[None]
        return carry

    lax.fori_loop(0, 9, owners, 0)
    send(6)
    pack(7, acc[0])
    arr[pl.ds(gx, 1), :, :] = msg[pl.ds(gx, 1), :, :]

    for q in range(1, GY):
        at = slice(q * KD, (q + 1) * KD)
        scol[at, :] = slots_of(quarter_of(ks_ref, q), gx) + q * KD
    send(7)

    dense[...] = jnp.zeros_like(dense)
    tal[...] = jnp.zeros_like(tal)
    hsum[...] = jnp.zeros_like(hsum)
    hcount[...] = jnp.zeros_like(hcount)
    lane8 = iota((8, W), 1)

    def arrive(m, carry):
        def wait(i, carry):
            s = pair_at(gx, -(i // 2), -offset(m)) + i % 2

            @pl.when(s != gx)
            def _():
                pltpu.make_async_remote_copy(
                    src_ref=msg.at[s], dst_ref=arr.at[s], send_sem=ssem.at[s],
                    recv_sem=rsem.at[s], device_id={"gx": s}, device_id_type=MESH,
                ).wait_recv()

            return carry

        lax.fori_loop(0, 8, wait, 0)
        for dx in range(4):
            pair = pair_at(gx, -dx, -offset(m))
            metas = []
            for i in range(2):
                s = pair + i

                q = arr[pl.ds(s, 1), 0:64, :][0].astype(I32)
                high = q >> 8
                at = slice((dx * 2 + i) * 64, (dx * 2 + i + 1) * 64)
                v_s[at, 0:W] = high.astype(F32).astype(BF16)
                v_s[at, W : 2 * W] = (q - high * 256).astype(F32).astype(BF16)
                tail = arr[pl.ds(s, 1), 64:80, :][0].astype(I32)
                meta = tail[8:16]
                hsum[...] += tail[0:8].astype(F32) * power(meta[:, 65:66].astype(F32))
                hcount[...] += meta[:, 64:65].astype(F32) + jnp.zeros((8, W), F32)
                metas.append(meta)
            meta_s[:, dx * W : (dx + 1) * W] = jnp.where(
                lane8 < 64, metas[0], pltpu.roll(metas[1], 64, 1)
            )
        meta = meta_s[...]
        scale = power(meta[2:3].astype(F32))
        count = meta[1:2].astype(F32)

        for q in range(GY):
            at = slice(q * KD, (q + 1) * KD)
            mine = scol[at, :] == meta[0:1]
            dense[at, :] += dot(jnp.where(mine, scale, 0.0).astype(BF16), v_s[...])
            hits = jnp.where(mine, count, 0.0)
            tal[at, :] += (hits[:, 0:W] + hits[:, W : 2 * W]) + (
                hits[:, 2 * W : 3 * W] + hits[:, 3 * W : 4 * W]
            )
        return carry

    lax.fori_loop(0, 8, arrive, 0)

    line8 = iota((8, W), 0)
    for q in range(GY):
        rows = jnp.where(line8 == 0, hsum[2 * q : 2 * q + 1], 0.0)
        rows = jnp.where(line8 == 1, hsum[2 * q + 1 : 2 * q + 2], rows)
        rows = jnp.where(line8 == 2, hcount[2 * q : 2 * q + 1], rows)
        rows = jnp.where(line8 == 3, hcount[2 * q + 1 : 2 * q + 2], rows)
        hquart[q, :, :] = rows

    def to_quarter(h, p):
        return pltpu.make_async_remote_copy(
            src_ref=quarters.at[h * GY + p], dst_ref=parts.at[h * GY + gy],
            send_sem=ysend.at[h * GY + p], recv_sem=yrecv.at[h * GY + gy],
            device_id={"gy": p}, device_id_type=MESH,
        )

    def heavy_to(p):
        return pltpu.make_async_remote_copy(
            src_ref=hquart.at[p], dst_ref=hparts.at[gy], send_sem=hsend.at[p],
            recv_sem=hrecv.at[gy], device_id={"gy": p}, device_id_type=MESH,
        )

    def leave(n, carry):
        h, k = n // GY, n % GY + 1
        p = (gy + k) % GY
        at = pl.ds(pl.multiple_of(p * KD + h * HK, HK), HK)
        q, e = encode(dense[at, 0:W] * 256.0 + dense[at, W : 2 * W])
        q = q.astype(I16)
        t = jnp.sum(tal[at, :].T, axis=0, keepdims=True)
        e = jnp.where(iota((HK, W), 1) == 0, e, 0.0).T[0:1]
        line = iota((16, W), 0)
        rows = jnp.zeros((16, W), F32)
        for i in range(2):
            rows = jnp.where(line == i, t[:, i * W : (i + 1) * W], rows)
            rows = jnp.where(line == 2 + i, e[:, i * W : (i + 1) * W], rows)
        rows = rows.astype(I32).astype(I16)
        quarters[pl.ds(h * GY + p, 1), 0:HK, :] = q[None]
        quarters[pl.ds(h * GY + p, 1), HK : HK + 16, :] = rows[None]

        @pl.when(k > 1)
        def _():
            to_quarter(h, (gy + k - 1) % GY).start()

        @pl.when(k == GY)
        def _():
            parts[pl.ds(h * GY + gy, 1), 0:HK, :] = q[None]
            parts[pl.ds(h * GY + gy, 1), HK : HK + 16, :] = rows[None]

        return carry

    lax.fori_loop(0, 2 * GY, leave, 0)
    for k in range(1, GY):
        heavy_to((gy + k) % GY).start()
    poscol[...] = slots_of(quarter_of(ks_ref, gy), gx)

    device = gx * GY + gy
    owners_here = [ks_ref[pl.ds(device * 4 + i, 1), :] >> 11 for i in range(4)]
    row = jnp.concatenate(owners_here, axis=1)
    square = jnp.zeros((W, W), I32)
    for i in range(4):
        square = jnp.where(iota((W, W), 0) == i, owners_here[i], square)
    square = square.astype(F32).T.astype(I32)
    col = jnp.concatenate([square[:, i : i + 1] for i in range(4)], axis=0)
    j0, j1 = iota((KD, KD), 0), iota((KD, KD), 1)
    w = jnp.sum(jnp.where((row == col) & (j1 < j0), 1.0, 0.0), axis=1, keepdims=True)
    place_s[...] = jnp.where(col * 8 + w.astype(I32) == j1, 1.0, 0.0).astype(BF16)

    def to_range(k, p):
        return pltpu.make_async_remote_copy(
            src_ref=scaled.at[k], dst_ref=moved.at[gx], send_sem=fsend.at[p],
            recv_sem=frecv.at[gx], device_id={"gx": p}, device_id_type=MESH,
        )

    slots_s[...] = jnp.zeros_like(slots_s)

    def half_quarter(h, carry):
        total, tallies = jnp.zeros((HK, W), F32), jnp.zeros((W, W), F32)
        for k in range(1, GY):
            s = (gy + GY - k) % GY
            pltpu.make_async_remote_copy(
                src_ref=quarters.at[h * GY + s], dst_ref=parts.at[h * GY + s],
                send_sem=ysend.at[h * GY + s], recv_sem=yrecv.at[h * GY + s],
                device_id={"gy": s}, device_id_type=MESH,
            ).wait_recv()
        for s in range(GY):
            rows = parts[pl.ds(h * GY + s, 1), HK : HK + 16, :][0].astype(F32)
            square = jnp.concatenate([rows, jnp.zeros((W - 16, W), F32)], axis=0).T
            scale = jnp.concatenate([square[:, 2 + i : 3 + i] for i in range(2)], axis=0)
            total = total + parts[pl.ds(h * GY + s, 1), 0:HK, :][0].astype(F32) * power(scale)
            tallies = tallies + square
        col = jnp.concatenate([tallies[:, i : i + 1] for i in range(2)], axis=0)
        at = pl.ds(pl.multiple_of(h * (GX // 2), GX // 2), GX // 2)
        scaled[at, :, :] = (total * lax.rsqrt(1.0 + col)).reshape(GX // 2, 8, W)
        pos = poscol[pl.ds(pl.multiple_of(h * HK, HK), HK), :]
        slots_s[...] += jnp.sum(
            jnp.where(pos == iota((HK, KD), 1), col, 0.0), axis=0, keepdims=True
        )

        def range_out(m, carry):
            for i in range(8):
                p = pair_at(gx, i // 2, offset(m)) + i % 2

                @pl.when(p != gx)
                def _():
                    to_range(m * 8 + i, p).start()

            return carry

        lax.fori_loop(h * 4, h * 4 + 4, range_out, 0)
        return carry

    lax.fori_loop(0, 2, half_quarter, 0)
    moved[pl.ds(gx, 1), :, :] = scaled[pl.ds(56 + gx % 2, 1), :, :]
    slots = slots_s[...]
    slots_ref[...] = jnp.concatenate([slots[:, i * W : (i + 1) * W] for i in range(4)], axis=0)
    tail = hquart[pl.ds(gy, 1), :, :][0]
    for k in range(1, GY):
        s = (gy + GY - k) % GY
        pltpu.make_async_remote_copy(
            src_ref=hquart.at[s], dst_ref=hparts.at[s], send_sem=hsend.at[s],
            recv_sem=hrecv.at[s], device_id={"gy": s}, device_id_type=MESH,
        ).wait_recv()
        tail = tail + hparts[pl.ds(s, 1), :, :][0]

    def finish(k, carry):
        s = (gx + k) % GX
        to_owner(s).wait_send()
        to_range(s, s).wait_send()
        pltpu.make_async_remote_copy(
            src_ref=scaled.at[s], dst_ref=moved.at[s], send_sem=fsend.at[s],
            recv_sem=frecv.at[s], device_id={"gx": s}, device_id_type=MESH,
        ).wait_recv()
        return carry

    lax.fori_loop(1, GX, finish, 0)
    for k in range(1, GY):
        to_quarter(0, (gy + k) % GY).wait_send()
        to_quarter(1, (gy + k) % GY).wait_send()
        heavy_to((gy + k) % GY).wait_send()

    inputs[4].wait()
    got = moved[...].reshape(KD, W)
    high = got.astype(BF16)
    low = (got - high.astype(F32)).astype(BF16)
    both = dot(place_s[...], jnp.concatenate([high, low], axis=1))
    total = both[:, 0:W] + both[:, W : 2 * W]
    orders = orders_ref[...].astype(F32)
    heavy = tail * lax.rsqrt(1.0 + pltpu.roll(tail, 6, 0))
    line = iota((KD, W), 0)
    reports = []
    for h in range(2):
        ours = iota((1, KD), 1) == 2 * device + h
        key = jnp.sum(jnp.where(ours, hk, 0).astype(F32), axis=1, keepdims=True).astype(I32)
        here = line == key - device * KD
        total = jnp.where(here, heavy[h : h + 1, :], total)
        mine = jnp.sum(jnp.where(here, orders, 0.0), axis=0, keepdims=True)
        reports.append(mine * heavy[h : h + 1, :])
    out_ref[...] = (orders * total).astype(BF16)
    report_ref[...] = jnp.concatenate(reports, axis=0).astype(BF16)


def join(keys, x, ks, heavy_keys, orders):
    rows = x.shape[0]
    chunks = rows // LANES
    dma = pltpu.SemaphoreType.DMA
    return pl.pallas_call(
        join_kernel,
        out_shape=(
            jax.ShapeDtypeStruct((KD, W), BF16),
            jax.ShapeDtypeStruct((2, W), BF16),
            jax.ShapeDtypeStruct((4, W), F32),
        ),
        in_specs=[pl.BlockSpec(memory_space=pl.ANY)] * 5,
        out_specs=(VMEM,) * 3,
        scratch_shapes=[
            pltpu.VMEM(keys.shape, I32),
            pltpu.VMEM(ks.shape, I32),
            pltpu.VMEM(heavy_keys.shape, I32),
            pltpu.VMEM(orders.shape, BF16),
            pltpu.VMEM((528, 512), BF16),
            pltpu.VMEM((chunks, LANES), I32),
            pltpu.VMEM((chunks, LANES), I32),
            pltpu.VMEM((chunks, LANES), I32),
            pltpu.VMEM((chunks, LANES), I32),
            pltpu.VMEM((rows, W), BF16),
            pltpu.VMEM((rows, W), BF16),
            pltpu.VMEM((rows, 2 * W), BF16),
            pltpu.VMEM((512, 256), F32),
            pltpu.VMEM((256, 512), BF16),
            pltpu.VMEM((2, 256, 2 * W), F32),
            pltpu.VMEM((2 * GX + 16, W), F32),
            pltpu.VMEM((GX, W), I32),
            pltpu.VMEM((GX, W), I32),
            pltpu.VMEM((512, W), I32),
            pltpu.VMEM((512, W), I32),
            pltpu.VMEM((GX, MSG, W), I16),
            pltpu.VMEM((GX, MSG, W), I16),
            pltpu.VMEM((512, 2 * W), BF16),
            pltpu.VMEM((8, 512), I32),
            pltpu.VMEM((OWN, 1), I32),
            pltpu.VMEM((OWN, 2 * W), F32),
            pltpu.VMEM((OWN, W), F32),
            pltpu.VMEM((8, W), F32),
            pltpu.VMEM((8, W), F32),
            pltpu.VMEM((2 * GY, HK + 16, W), I16),
            pltpu.VMEM((2 * GY, HK + 16, W), I16),
            pltpu.VMEM((GY, 8, W), F32),
            pltpu.VMEM((GY, 8, W), F32),
            pltpu.VMEM((GX, 8, W), F32),
            pltpu.VMEM((GX, 8, W), F32),
            pltpu.VMEM((KD, KD), BF16),
            pltpu.VMEM((KD, 1), I32),
            pltpu.VMEM((1, KD), F32),
            dma((GX,)), dma((GX,)), dma((2 * GY,)), dma((2 * GY,)), dma((GY,)), dma((GY,)),
            dma((GX,)), dma((GX,)), dma((5,)),
        ],
        compiler_params=pltpu.CompilerParams(
            collective_id=0, has_side_effects=True, vmem_limit_bytes=56 * 2**20
        ),
        name="join_rows",
    )(keys, x, ks, heavy_keys, orders)


def hand_on_kernel(a_ref, b_ref, c_ref, out_a, out_b, out_c):
    out_a[...] = a_ref[...]
    out_b[...] = b_ref[...]
    out_c[...] = c_ref[...]


def hand_on(*arrays):
    return pl.pallas_call(
        hand_on_kernel,
        out_shape=tuple(jax.ShapeDtypeStruct(a.shape, a.dtype) for a in arrays),
        in_specs=[VMEM] * 3,
        out_specs=(VMEM,) * 3,
        name="hand_on",
    )(*arrays)


def body(measures, row_keys, orders, heavy_keys, key_slot):
    result, report, slot_rows = join(
        row_keys.reshape(-1, W), measures, key_slot.reshape(-1, W), heavy_keys.reshape(-1, W), orders
    )
    result, report, slot_rows = hand_on(result, report, slot_rows)
    return (result, report, slot_rows.reshape(KD))


def solution(mesh):
    return jax.shard_map(
        body,
        mesh=mesh,
        in_specs=(P(("gx", "gy"), None), P(("gx", "gy")), P(("gx", "gy"), None), P(), P()),
        out_specs=(P(("gx", "gy"), None), P(("gx", "gy"), None), P(("gx", "gy"))),
        check_vma=False,
    )
```

```python
import jax
import jax.numpy as jnp
from jax import lax
from jax.experimental import pallas as pl
from jax.experimental.pallas import tpu as pltpu
from jax.sharding import PartitionSpec as P

MESH = pl.DeviceIdType.MESH
F32, BF16, I32, I16 = jnp.float32, jnp.bfloat16, jnp.int32, jnp.int16
LN2 = 0.6931471805599453

W = 128
GX, GY = 64, 4
KEYS = 131072
KD = 512
HK = 128
NP = KD // HK
OWN = 2048
CAPK = 64
HALF = 2048
HG = 8
MSG = 80
LANES = 1024
VMEM = pl.BlockSpec(memory_space=pltpu.VMEM)


def iota(shape, dim):
    return lax.broadcasted_iota(I32, shape, dim)


def onehot(rows, lanes, base, labels):
    labels = (labels - base).astype(I16)
    return jnp.where(iota((rows, lanes), 0).astype(I16) == labels, jnp.ones((), BF16), jnp.zeros((), BF16))


def dot(a, b):
    return jnp.dot(a, b, preferred_element_type=F32)


def dot_t(a, b):
    return lax.dot_general(a, b, (((1,), (1,)), ((), ())), preferred_element_type=F32)


def power(e):
    return jnp.exp(e * LN2)


def encode(v):
    top = jnp.max(jnp.abs(v), axis=1, keepdims=True)
    e = jnp.ceil(jnp.log(jnp.maximum(top, 1e-30)) * (1.0 / LN2) - 14.99)
    e = jnp.maximum(e, -100.0)
    q = jnp.floor(v * power(-e) + 0.5).astype(I32)
    return q, e


def quarter_of(ks_ref, q):
    rows = [ks_ref[pl.ds(q * 4 + i, GX, stride=16), :] for i in range(4)]
    return jnp.concatenate(rows, axis=1)


def slots_of(ks, me):
    mine = jnp.where((ks >> 11) == me, 1.0, 0.0)
    upper = jnp.where(iota((KD, KD), 0) < iota((KD, KD), 1), 1.0, 0.0).astype(BF16)
    w = dot(mine.astype(BF16), upper)
    pos = (ks & (KD - 1)).astype(F32)
    lane = iota((GX, W), 1)
    table = jnp.zeros((GX, W), F32)
    for k in range(8):
        s = jnp.sum(jnp.where((mine > 0.5) & (w == float(k)), pos, 0.0), axis=1, keepdims=True)
        table = jnp.where(lane == k, s, table)
    high = jnp.floor(table * (1.0 / 256.0))
    low = table - 256.0 * high
    place = iota((KD, GX), 0) >> 3
    zi = 7 - (place >> 3)
    dz = ((zi + 1) >> 1) * (1 - 2 * ((zi + 1) & 1))
    z, x = (me // 2) % 8 + 8 + dz, me // 16 + ((place >> 1) & 3)
    block = ((x & 3) * 8 + (z & 7)) * 2 + (place & 1)
    repeat = jnp.where(block == iota((KD, GX), 1), 1.0, 0.0).astype(BF16)
    each = 256.0 * dot(repeat, high.astype(BF16)) + dot(repeat, low.astype(BF16))
    pick = iota((KD, W), 1) == (iota((KD, W), 0) & 7)
    return jnp.sum(jnp.where(pick, each, 0.0), axis=1, keepdims=True).astype(I32)


def offset(m):
    zi = 7 - m
    return ((zi + 1) // 2) * (1 - 2 * ((zi + 1) % 2))


def pair_at(me, dx, dz):
    z, x = (me // 2) % 8, me // 16
    return (((x + 4 + dx) % 4) * 8 + (z + 8 + dz) % 8) * 2


def join_kernel(keys_in, x_in, ks_in, hk_in, orders_in,
                out_ref, report_ref, slots_ref,
                keys_ref, ks_ref, hk_ref, orders_ref, tab, shi_s, slo_s, seg_s, run_s, xin, xm, xe, pt, rk, acc, ext, cnt_s, slot_s,
                hq, hx, msg, arr,
                v_s, meta_s, scol, dense, tal, hsum, hcount, quarters, parts, hquart, hparts,
                scaled, moved, place_s, poscol, slots_s, ssem, rsem, ysend, yrecv, hsend, hrecv, fsend, frecv, isem):
    gx, gy = lax.axis_index("gx"), lax.axis_index("gy")
    barrier = pltpu.get_barrier_semaphore()
    pairs = ((ks_in, ks_ref), (hk_in, hk_ref), (keys_in, keys_ref), (x_in, xin), (orders_in, orders_ref))
    inputs = [pltpu.make_async_copy(a, b, isem.at[i]) for i, (a, b) in enumerate(pairs)]
    for copy in inputs:
        copy.start()

    def greet(m, carry):
        for i in range(8):
            p = pair_at(gx, i // 2, offset(m)) + i % 2

            @pl.when(p != gx)
            def _():
                pl.semaphore_signal(barrier, inc=1, device_id={"gx": p}, device_id_type=MESH)

        return carry

    lax.fori_loop(0, 8, greet, 0)
    for k in range(1, GY):
        pl.semaphore_signal(barrier, inc=1, device_id={"gy": (gy + k) % GY}, device_id_type=MESH)

    chunks = xe.shape[0] // LANES
    hi_n, lo_n = 512, 256
    inputs[0].wait()
    inputs[1].wait()
    for i in range(2):
        ks = ks_ref[pl.ds(i, hi_n, stride=2), :]
        p1 = (ks >> 11) * 2 + ((ks >> 8) & 1)
        tab[i * W : (i + 1) * W, :] = p1.astype(F32).T.astype(BF16)
        tab[lo_n + i * W : lo_n + (i + 1) * W, :] = (ks & 255).astype(F32).T.astype(BF16)
    hk = jnp.concatenate([hk_ref[i : i + 1, :] for i in range(4)], axis=1)
    line = iota((16, hi_n), 0)
    digits = jnp.where(line == 0, hk & 255, jnp.where(line == 1, (hk >> 8) & 1, 0))
    digits = digits.astype(F32).astype(BF16)
    block = 2 * (iota((hi_n, hi_n), 1) >> 1)
    odd = (iota((1, hi_n), 1) & 1).astype(F32)
    marks = jnp.full((16, hi_n), -1.0, F32)
    for i in range(2):
        pick = jnp.where(iota((hi_n, hi_n), 0) == block + i, 1.0, 0.0).astype(BF16)
        found = dot(digits, pick)
        marks = jnp.where(line == i, jnp.where(found[1:2] == odd, found[0:1], -1.0), marks)
    tab[2 * lo_n : 2 * lo_n + 16, :] = marks.astype(BF16)
    z0, x0 = (gx // 2) % 8, gx // 16
    pt[...] = jnp.zeros_like(pt)

    def look(c, carry):
        block = keys_ref[pl.ds(pl.multiple_of(c * 8, 8), 8), :]
        key = jnp.concatenate([block[i : i + 1] for i in range(8)], axis=1)
        hi, lo = key >> 8, key & 255
        t = dot(tab[...], onehot(hi_n, LANES, 0, hi))
        mine = iota((lo_n, LANES), 0) == lo
        a = jnp.sum(jnp.where(mine, t[:lo_n], 0.0), axis=0, keepdims=True).astype(I32)
        b = jnp.sum(jnp.where(mine, t[lo_n : 2 * lo_n], 0.0), axis=0, keepdims=True).astype(I32)
        low = lo.astype(F32)
        second = t[2 * lo_n + 1 : 2 * lo_n + 2] == low
        heavy = (t[2 * lo_n : 2 * lo_n + 1] == low) | second
        owner = a >> 1
        dx = ((owner >> 4) + 4 - x0) & 3
        dz = (((owner >> 1) & 7) + 8 - z0) & 7
        zi = jnp.where(dz == 0, 0, jnp.where(dz <= 4, 2 * dz - 1, 16 - 2 * dz))
        place = (7 - zi) * 8 + dx * 2 + (owner & 1)
        shi = jnp.where(heavy, -1, owner * 8 + ((key >> 9) & 3) * 2 + (a & 1))
        shi_s[pl.ds(c, 1), :] = shi
        slo_s[pl.ds(c, 1), :] = b
        hid = (key >> 9) * 2 + jnp.where(second, 1, 0)
        seg_s[pl.ds(c, 1), :] = jnp.where(heavy, HALF + (hid & 255), (place >> 1) * CAPK)
        run_s[pl.ds(c, 1), :] = jnp.where(heavy, 2 * GX + (hid >> 5), (place >> 5) * CAPK)
        sub = jnp.where(heavy, hid, place) & 31
        line = iota((W, LANES), 0)
        kind = line >> 5
        facts = jnp.where(kind == 0, 1, jnp.where(kind == 1, b, jnp.where(kind == 2, shi & 7, 0)))
        facts = jnp.where((line & 31) == sub, facts, 0)
        at = pl.ds(pl.multiple_of(c * LANES, LANES), LANES)
        xm[at, :] = facts.astype(F32).T.astype(BF16)
        side = jnp.where(heavy, hid >> 8, place & 1).astype(F32)
        sides = jnp.broadcast_to(side, (W, LANES)).T.astype(BF16)
        x = xin[at, :]
        right = x * sides
        xe[at, 0:W] = x - right
        xe[at, W : 2 * W] = right
        pt[...] += dot_t(onehot(hi_n, LANES, 0, shi), onehot(lo_n, LANES, 0, b))
        return carry

    inputs[2].wait()
    inputs[3].wait()
    lax.fori_loop(0, chunks, look, 0, unroll=4)

    here = jnp.where(pt[...] > 0.5, 1.0, 0.0).T.astype(BF16)
    lower = jnp.where(iota((lo_n, lo_n), 1) < iota((lo_n, lo_n), 0), 1.0, 0.0).astype(BF16)
    r0, r1 = iota((hi_n, hi_n), 0), iota((hi_n, hi_n), 1)
    before = jnp.where((r0 < r1) & ((r0 >> 3) == (r1 >> 3)), 1.0, 0.0).astype(BF16)
    column = dot(jnp.ones((lo_n, lo_n), BF16), here).astype(BF16)
    rk[...] = (dot(lower, here) + dot(column, before)).astype(BF16)

    def rank(c, carry):
        shi = shi_s[pl.ds(c, 1), :]
        slo = slo_s[pl.ds(c, 1), :]
        t = dot(rk[...], onehot(hi_n, LANES, 0, shi))
        mine = iota((lo_n, LANES), 0) == slo
        r = jnp.sum(jnp.where(mine, t, 0.0), axis=0, keepdims=True).astype(I32)
        r = jnp.where(shi < 0, 0, r)
        seg_s[pl.ds(c, 1), :] = seg_s[pl.ds(c, 1), :] + r
        run_s[pl.ds(c, 1), :] = run_s[pl.ds(c, 1), :] + r
        return carry

    lax.fori_loop(0, chunks, rank, 0, unroll=4)

    def sums(base):
        total = None
        for c in range(chunks):
            at = slice(c * LANES, (c + 1) * LANES)
            part = dot(onehot(256, LANES, base, seg_s[c : c + 1, :]), xe[at, :])
            total = part if total is None else total + part
        return total

    ext[...] = jnp.zeros_like(ext)

    def gather_facts(c, carry):
        at = pl.ds(pl.multiple_of(c * LANES, LANES), LANES)
        ext[...] += dot(onehot(2 * GX + 16, LANES, 0, run_s[pl.ds(c, 1), :]), xm[at, :])
        return carry

    lax.fori_loop(0, chunks, gather_facts, 0, unroll=4)
    square = ext[0 : 2 * GX, :].T
    cnt = square[0:32]
    slot = jnp.floor((square[32:64] + 256.0 * square[64:96]) / jnp.maximum(cnt, 1.0) + 0.5)
    slot = jnp.where(cnt > 0.5, slot, -1.0)
    cnt_s[0:32, :] = cnt.astype(I32)
    cnt_s[32:64, :] = pltpu.roll(cnt, 64, 1).astype(I32)
    slot_s[0:32, :] = slot.astype(I32)
    slot_s[32:64, :] = pltpu.roll(slot, 64, 1).astype(I32)

    lane = iota((512, W), 1)
    counts = ext[2 * GX : 2 * GX + 16, :]
    high = jnp.floor(counts * (1.0 / 256.0))
    spread = jnp.where((iota((512, 16), 0) >> 5) == iota((512, 16), 1), 1.0, 0.0).astype(BF16)
    each = 256.0 * dot(spread, high.astype(BF16)) + dot(spread, (counts - 256.0 * high).astype(BF16))
    pick = lane == (iota((512, W), 0) & 31)
    counts = jnp.sum(jnp.where(pick, each, 0.0), axis=1, keepdims=True)

    def pack_heavy():
        both = acc[0]
        q, e = encode(jnp.concatenate([both[:, 0:W], both[:, W : 2 * W]], axis=0))
        hq[...] = q
        hx[...] = jnp.where(lane == 64, counts, jnp.where(lane == 65, e, 0.0)).astype(I32)

    acc[...] = jnp.zeros_like(acc)
    hq[...] = jnp.zeros_like(hq)
    hx[...] = jnp.zeros_like(hx)
    pl.semaphore_wait(barrier, GX + GY - 2)

    def to_owner(o):
        return pltpu.make_async_remote_copy(
            src_ref=msg.at[o], dst_ref=arr.at[gx], send_sem=ssem.at[o], recv_sem=rsem.at[gx],
            device_id={"gx": o}, device_id_type=MESH,
        )

    def send(m):
        for i in range(8):
            o = pair_at(gx, i // 2, offset(m)) + i % 2

            @pl.when(o != gx)
            def _():
                to_owner(o).start()

    def pack(m, both):
        q0, e0 = encode(both[:, 0:W])
        q1, e1 = encode(both[:, W : 2 * W])
        lane = iota((256, W), 1)
        e = jnp.where(lane == 0, e0, jnp.where(lane == 1, e1, 0.0)).T[0:8].astype(I32)
        pairs = [pair_at(gx, dx, offset(m)) for dx in range(4)]
        at = pl.ds(pl.multiple_of(m * 8, 8), 8)
        slots, counts = slot_s[at, :], cnt_s[at, :]
        lane, line = iota((8, W), 1), iota((8, W), 0)
        for i in range(8):
            o = pairs[i // 2] + i % 2
            part = e[i % 2 : i % 2 + 1, (i // 4) * W : (i // 4 + 1) * W]
            exps = pltpu.roll(part, 64, 1) if (i // 2) % 2 else part
            meta = jnp.where(line == 0, slots[i : i + 1], jnp.where(line == 1, counts[i : i + 1], exps))
            at = pl.ds(pl.multiple_of(o * 8, 8), 8)
            meta = jnp.where(lane < 64, meta, hx[at, :])
            values = (q1 if i % 2 else q0)[(i // 2) * 64 : (i // 2 + 1) * 64]
            msg[pl.ds(o, 1), 0:64, :] = values.astype(I16)[None]
            tail = jnp.concatenate([hq[at, :], meta], axis=0).astype(I16)
            msg[pl.ds(o, 1), 64:80, :] = tail[None]

    def owners(t, carry):
        @pl.when(t == 1)
        def _():
            pack_heavy()

        @pl.when(t == 2)
        def _():
            pack(0, acc[1])
            scol[0:KD, :] = slots_of(quarter_of(ks_ref, 0), gx)
            send(0)

        @pl.when(t > 3)
        def _():
            send(t - 3)

        pack(jnp.maximum(t - 2, 1), acc[pl.ds((t + 1) % 2, 1), :, :][0])
        acc[pl.ds(t % 2, 1), :, :] = sums(((t + 8) % 9) * 256)[None]
        return carry

    lax.fori_loop(0, 9, owners, 0)
    send(6)
    pack(7, acc[0])
    arr[pl.ds(gx, 1), :, :] = msg[pl.ds(gx, 1), :, :]

    for q in range(1, GY):
        at = slice(q * KD, (q + 1) * KD)
        scol[at, :] = slots_of(quarter_of(ks_ref, q), gx) + q * KD
    send(7)

    dense[...] = jnp.zeros_like(dense)
    tal[...] = jnp.zeros_like(tal)
    hsum[...] = jnp.zeros_like(hsum)
    hcount[...] = jnp.zeros_like(hcount)
    lane8 = iota((8, W), 1)

    def arrive(m, carry):
        def wait(i, carry):
            s = pair_at(gx, -(i // 2), -offset(m)) + i % 2

            @pl.when(s != gx)
            def _():
                pltpu.make_async_remote_copy(
                    src_ref=msg.at[s], dst_ref=arr.at[s], send_sem=ssem.at[s],
                    recv_sem=rsem.at[s], device_id={"gx": s}, device_id_type=MESH,
                ).wait_recv()

            return carry

        lax.fori_loop(0, 8, wait, 0)
        for dx in range(4):
            pair = pair_at(gx, -dx, -offset(m))
            metas = []
            for i in range(2):
                s = pair + i

                q = arr[pl.ds(s, 1), 0:64, :][0].astype(I32)
                high = q >> 8
                at = slice((dx * 2 + i) * 64, (dx * 2 + i + 1) * 64)
                v_s[at, 0:W] = high.astype(F32).astype(BF16)
                v_s[at, W : 2 * W] = (q - high * 256).astype(F32).astype(BF16)
                tail = arr[pl.ds(s, 1), 64:80, :][0].astype(I32)
                meta = tail[8:16]
                hsum[...] += tail[0:8].astype(F32) * power(meta[:, 65:66].astype(F32))
                hcount[...] += meta[:, 64:65].astype(F32) + jnp.zeros((8, W), F32)
                metas.append(meta)
            meta_s[:, dx * W : (dx + 1) * W] = jnp.where(
                lane8 < 64, metas[0], pltpu.roll(metas[1], 64, 1)
            )
        meta = meta_s[...]
        scale = power(meta[2:3].astype(F32))
        count = meta[1:2].astype(F32)

        for q in range(GY):
            at = slice(q * KD, (q + 1) * KD)
            mine = scol[at, :] == meta[0:1]
            dense[at, :] += dot(jnp.where(mine, scale, 0.0).astype(BF16), v_s[...])
            hits = jnp.where(mine, count, 0.0)
            tal[at, :] += (hits[:, 0:W] + hits[:, W : 2 * W]) + (
                hits[:, 2 * W : 3 * W] + hits[:, 3 * W : 4 * W]
            )
        return carry

    lax.fori_loop(0, 8, arrive, 0)

    line8 = iota((8, W), 0)
    for q in range(GY):
        rows = jnp.where(line8 == 0, hsum[2 * q : 2 * q + 1], 0.0)
        rows = jnp.where(line8 == 1, hsum[2 * q + 1 : 2 * q + 2], rows)
        rows = jnp.where(line8 == 2, hcount[2 * q : 2 * q + 1], rows)
        rows = jnp.where(line8 == 3, hcount[2 * q + 1 : 2 * q + 2], rows)
        hquart[q, :, :] = rows

    def to_quarter(h, p):
        return pltpu.make_async_remote_copy(
            src_ref=quarters.at[h * GY + p], dst_ref=parts.at[h * GY + gy],
            send_sem=ysend.at[h * GY + p], recv_sem=yrecv.at[h * GY + gy],
            device_id={"gy": p}, device_id_type=MESH,
        )

    def heavy_to(p):
        return pltpu.make_async_remote_copy(
            src_ref=hquart.at[p], dst_ref=hparts.at[gy], send_sem=hsend.at[p],
            recv_sem=hrecv.at[gy], device_id={"gy": p}, device_id_type=MESH,
        )

    def leave(n, carry):
        h, k = n // GY, n % GY + 1
        p = (gy + k) % GY
        at = pl.ds(pl.multiple_of(p * KD + h * HK, HK), HK)
        q, e = encode(dense[at, 0:W] * 256.0 + dense[at, W : 2 * W])
        q = q.astype(I16)
        t = jnp.sum(tal[at, :].T, axis=0, keepdims=True)
        e = jnp.where(iota((HK, W), 1) == 0, e, 0.0).T[0:1]
        line = iota((16, W), 0)
        rows = jnp.zeros((16, W), F32)
        rows = jnp.where(line == 0, t, jnp.where(line == 1, e, rows))
        rows = rows.astype(I32).astype(I16)
        quarters[pl.ds(h * GY + p, 1), 0:HK, :] = q[None]
        quarters[pl.ds(h * GY + p, 1), HK : HK + 16, :] = rows[None]

        @pl.when(k > 1)
        def _():
            to_quarter(h, (gy + k - 1) % GY).start()

        @pl.when(k == GY)
        def _():
            parts[pl.ds(h * GY + gy, 1), 0:HK, :] = q[None]
            parts[pl.ds(h * GY + gy, 1), HK : HK + 16, :] = rows[None]

        return carry

    lax.fori_loop(0, NP * GY, leave, 0)
    for k in range(1, GY):
        heavy_to((gy + k) % GY).start()
    poscol[...] = slots_of(quarter_of(ks_ref, gy), gx)

    device = gx * GY + gy
    owners_here = [ks_ref[pl.ds(device * 4 + i, 1), :] >> 11 for i in range(4)]
    row = jnp.concatenate(owners_here, axis=1)
    square = jnp.zeros((W, W), I32)
    for i in range(4):
        square = jnp.where(iota((W, W), 0) == i, owners_here[i], square)
    square = square.astype(F32).T.astype(I32)
    col = jnp.concatenate([square[:, i : i + 1] for i in range(4)], axis=0)
    j0, j1 = iota((KD, KD), 0), iota((KD, KD), 1)
    w = jnp.sum(jnp.where((row == col) & (j1 < j0), 1.0, 0.0), axis=1, keepdims=True)
    place_s[...] = jnp.where(col * 8 + w.astype(I32) == j1, 1.0, 0.0).astype(BF16)

    def to_range(k, p):
        return pltpu.make_async_remote_copy(
            src_ref=scaled.at[k], dst_ref=moved.at[gx], send_sem=fsend.at[p],
            recv_sem=frecv.at[gx], device_id={"gx": p}, device_id_type=MESH,
        )

    slots_s[...] = jnp.zeros_like(slots_s)

    def piece(h, carry):
        total, tallies = jnp.zeros((HK, W), F32), jnp.zeros((W, W), F32)
        for k in range(1, GY):
            s = (gy + GY - k) % GY
            pltpu.make_async_remote_copy(
                src_ref=quarters.at[h * GY + s], dst_ref=parts.at[h * GY + s],
                send_sem=ysend.at[h * GY + s], recv_sem=yrecv.at[h * GY + s],
                device_id={"gy": s}, device_id_type=MESH,
            ).wait_recv()
        for s in range(GY):
            rows = parts[pl.ds(h * GY + s, 1), HK : HK + 16, :][0].astype(F32)
            square = jnp.concatenate([rows, jnp.zeros((W - 16, W), F32)], axis=0).T
            scale = square[:, 1:2]
            total = total + parts[pl.ds(h * GY + s, 1), 0:HK, :][0].astype(F32) * power(scale)
            tallies = tallies + square
        col = tallies[:, 0:1]
        at = pl.ds(h * (GX // NP), GX // NP)
        scaled[at, :, :] = (total * lax.rsqrt(1.0 + col)).reshape(GX // NP, 8, W)
        pos = poscol[pl.ds(pl.multiple_of(h * HK, HK), HK), :]
        slots_s[...] += jnp.sum(
            jnp.where(pos == iota((HK, KD), 1), col, 0.0), axis=0, keepdims=True
        )

        def range_out(m, carry):
            for i in range(8):
                p = pair_at(gx, i // 2, offset(m)) + i % 2

                @pl.when(p != gx)
                def _():
                    to_range(m * 8 + i, p).start()

            return carry

        lax.fori_loop(h * (8 // NP), (h + 1) * (8 // NP), range_out, 0)
        return carry

    lax.fori_loop(0, NP, piece, 0)
    moved[pl.ds(gx, 1), :, :] = scaled[pl.ds(56 + gx % 2, 1), :, :]
    slots = slots_s[...]
    slots_ref[...] = jnp.concatenate([slots[:, i * W : (i + 1) * W] for i in range(4)], axis=0)
    tail = hquart[pl.ds(gy, 1), :, :][0]
    for k in range(1, GY):
        s = (gy + GY - k) % GY
        pltpu.make_async_remote_copy(
            src_ref=hquart.at[s], dst_ref=hparts.at[s], send_sem=hsend.at[s],
            recv_sem=hrecv.at[s], device_id={"gy": s}, device_id_type=MESH,
        ).wait_recv()
        tail = tail + hparts[pl.ds(s, 1), :, :][0]

    def finish(k, carry):
        s = (gx + k) % GX
        to_owner(s).wait_send()
        to_range(s, s).wait_send()
        pltpu.make_async_remote_copy(
            src_ref=scaled.at[s], dst_ref=moved.at[s], send_sem=fsend.at[s],
            recv_sem=frecv.at[s], device_id={"gx": s}, device_id_type=MESH,
        ).wait_recv()
        return carry

    lax.fori_loop(1, GX, finish, 0)
    for k in range(1, GY):
        for h in range(NP):
            to_quarter(h, (gy + k) % GY).wait_send()
        heavy_to((gy + k) % GY).wait_send()

    inputs[4].wait()
    got = moved[...].reshape(KD, W)
    high = got.astype(BF16)
    low = (got - high.astype(F32)).astype(BF16)
    both = dot(place_s[...], jnp.concatenate([high, low], axis=1))
    total = both[:, 0:W] + both[:, W : 2 * W]
    orders = orders_ref[...].astype(F32)
    heavy = tail * lax.rsqrt(1.0 + pltpu.roll(tail, 6, 0))
    line = iota((KD, W), 0)
    reports = []
    for h in range(2):
        ours = iota((1, KD), 1) == 2 * device + h
        key = jnp.sum(jnp.where(ours, hk, 0).astype(F32), axis=1, keepdims=True).astype(I32)
        here = line == key - device * KD
        total = jnp.where(here, heavy[h : h + 1, :], total)
        mine = jnp.sum(jnp.where(here, orders, 0.0), axis=0, keepdims=True)
        reports.append(mine * heavy[h : h + 1, :])
    out_ref[...] = (orders * total).astype(BF16)
    report_ref[...] = jnp.concatenate(reports, axis=0).astype(BF16)


def join(keys, x, ks, heavy_keys, orders):
    rows = x.shape[0]
    chunks = rows // LANES
    dma = pltpu.SemaphoreType.DMA
    return pl.pallas_call(
        join_kernel,
        out_shape=(
            jax.ShapeDtypeStruct((KD, W), BF16),
            jax.ShapeDtypeStruct((2, W), BF16),
            jax.ShapeDtypeStruct((4, W), F32),
        ),
        in_specs=[pl.BlockSpec(memory_space=pl.ANY)] * 5,
        out_specs=(VMEM,) * 3,
        scratch_shapes=[
            pltpu.VMEM(keys.shape, I32),
            pltpu.VMEM(ks.shape, I32),
            pltpu.VMEM(heavy_keys.shape, I32),
            pltpu.VMEM(orders.shape, BF16),
            pltpu.VMEM((528, 512), BF16),
            pltpu.VMEM((chunks, LANES), I32),
            pltpu.VMEM((chunks, LANES), I32),
            pltpu.VMEM((chunks, LANES), I32),
            pltpu.VMEM((chunks, LANES), I32),
            pltpu.VMEM((rows, W), BF16),
            pltpu.VMEM((rows, W), BF16),
            pltpu.VMEM((rows, 2 * W), BF16),
            pltpu.VMEM((512, 256), F32),
            pltpu.VMEM((256, 512), BF16),
            pltpu.VMEM((2, 256, 2 * W), F32),
            pltpu.VMEM((2 * GX + 16, W), F32),
            pltpu.VMEM((GX, W), I32),
            pltpu.VMEM((GX, W), I32),
            pltpu.VMEM((512, W), I32),
            pltpu.VMEM((512, W), I32),
            pltpu.VMEM((GX, MSG, W), I16),
            pltpu.VMEM((GX, MSG, W), I16),
            pltpu.VMEM((512, 2 * W), BF16),
            pltpu.VMEM((8, 512), I32),
            pltpu.VMEM((OWN, 1), I32),
            pltpu.VMEM((OWN, 2 * W), F32),
            pltpu.VMEM((OWN, W), F32),
            pltpu.VMEM((8, W), F32),
            pltpu.VMEM((8, W), F32),
            pltpu.VMEM((NP * GY, HK + 16, W), I16),
            pltpu.VMEM((NP * GY, HK + 16, W), I16),
            pltpu.VMEM((GY, 8, W), F32),
            pltpu.VMEM((GY, 8, W), F32),
            pltpu.VMEM((GX, 8, W), F32),
            pltpu.VMEM((GX, 8, W), F32),
            pltpu.VMEM((KD, KD), BF16),
            pltpu.VMEM((KD, 1), I32),
            pltpu.VMEM((1, KD), F32),
            dma((GX,)), dma((GX,)), dma((NP * GY,)), dma((NP * GY,)), dma((GY,)), dma((GY,)),
            dma((GX,)), dma((GX,)), dma((5,)),
        ],
        compiler_params=pltpu.CompilerParams(
            collective_id=0, has_side_effects=True, vmem_limit_bytes=56 * 2**20
        ),
        name="join_rows",
    )(keys, x, ks, heavy_keys, orders)


def hand_on_kernel(a_ref, b_ref, c_ref, out_a, out_b, out_c):
    out_a[...] = a_ref[...]
    out_b[...] = b_ref[...]
    out_c[...] = c_ref[...]


def hand_on(*arrays):
    return pl.pallas_call(
        hand_on_kernel,
        out_shape=tuple(jax.ShapeDtypeStruct(a.shape, a.dtype) for a in arrays),
        in_specs=[VMEM] * 3,
        out_specs=(VMEM,) * 3,
        name="hand_on",
    )(*arrays)


def body(measures, row_keys, orders, heavy_keys, key_slot):
    result, report, slot_rows = join(
        row_keys.reshape(-1, W), measures, key_slot.reshape(-1, W), heavy_keys.reshape(-1, W), orders
    )
    result, report, slot_rows = hand_on(result, report, slot_rows)
    return (result, report, slot_rows.reshape(KD))


def solution(mesh):
    return jax.shard_map(
        body,
        mesh=mesh,
        in_specs=(P(("gx", "gy"), None), P(("gx", "gy")), P(("gx", "gy"), None), P(), P()),
        out_specs=(P(("gx", "gy"), None), P(("gx", "gy"), None), P(("gx", "gy"))),
        check_vma=False,
    )
```

```python
import jax
import jax.numpy as jnp
from jax import lax
from jax.experimental import pallas as pl
from jax.experimental.pallas import tpu as pltpu
from jax.sharding import PartitionSpec as P

MESH = pl.DeviceIdType.MESH
F32, BF16, I32, I16 = jnp.float32, jnp.bfloat16, jnp.int32, jnp.int16
LN2 = 0.6931471805599453

W = 128
GX, GY = 64, 4
KEYS = 131072
KD = 512
HK = 128
NP = KD // HK
OWN = 2048
CAPK = 64
HALF = 2048
HG = 8
MSG = 80
LANES = 1024
VMEM = pl.BlockSpec(memory_space=pltpu.VMEM)


def iota(shape, dim):
    return lax.broadcasted_iota(I32, shape, dim)


def onehot(rows, lanes, base, labels):
    labels = (labels - base).astype(I16)
    return jnp.where(iota((rows, lanes), 0).astype(I16) == labels, jnp.ones((), BF16), jnp.zeros((), BF16))


def dot(a, b):
    return jnp.dot(a, b, preferred_element_type=F32)


def dot_t(a, b):
    return lax.dot_general(a, b, (((1,), (1,)), ((), ())), preferred_element_type=F32)


def power(e):
    return jnp.exp(e * LN2)


def encode(v):
    top = jnp.max(jnp.abs(v), axis=1, keepdims=True)
    e = jnp.ceil(jnp.log(jnp.maximum(top, 1e-30)) * (1.0 / LN2) - 14.99)
    e = jnp.maximum(e, -100.0)
    q = jnp.floor(v * power(-e) + 0.5).astype(I32)
    return q, e


def quarter_of(ks_ref, q):
    rows = [ks_ref[pl.ds(q * 4 + i, GX, stride=16), :] for i in range(4)]
    return jnp.concatenate(rows, axis=1)


def slots_of(ks, me):
    mine = jnp.where((ks >> 11) == me, 1.0, 0.0)
    upper = jnp.where(iota((KD, KD), 0) < iota((KD, KD), 1), 1.0, 0.0).astype(BF16)
    w = dot(mine.astype(BF16), upper)
    pos = (ks & (KD - 1)).astype(F32)
    lane = iota((GX, W), 1)
    table = jnp.zeros((GX, W), F32)
    for k in range(8):
        s = jnp.sum(jnp.where((mine > 0.5) & (w == float(k)), pos, 0.0), axis=1, keepdims=True)
        table = jnp.where(lane == k, s, table)
    high = jnp.floor(table * (1.0 / 256.0))
    low = table - 256.0 * high
    place = iota((KD, GX), 0) >> 3
    zi = 7 - (place >> 3)
    dz = ((zi + 1) >> 1) * (1 - 2 * ((zi + 1) & 1))
    z, x = (me // 2) % 8 + 8 + dz, me // 16 + ((place >> 1) & 3)
    block = ((x & 3) * 8 + (z & 7)) * 2 + (place & 1)
    repeat = jnp.where(block == iota((KD, GX), 1), 1.0, 0.0).astype(BF16)
    each = 256.0 * dot(repeat, high.astype(BF16)) + dot(repeat, low.astype(BF16))
    pick = iota((KD, W), 1) == (iota((KD, W), 0) & 7)
    return jnp.sum(jnp.where(pick, each, 0.0), axis=1, keepdims=True).astype(I32)


def offset(m):
    zi = 7 - m
    return ((zi + 1) // 2) * (1 - 2 * ((zi + 1) % 2))


def pair_at(me, dx, dz):
    z, x = (me // 2) % 8, me // 16
    return (((x + 4 + dx) % 4) * 8 + (z + 8 + dz) % 8) * 2


def join_kernel(keys_in, x_in, ks_in, hk_in, orders_in,
                out_ref, report_ref, slots_ref,
                keys_ref, ks_ref, hk_ref, orders_ref, tab, shi_s, slo_s, seg_s, run_s, xin, xm, xe, pt, rk, acc, ext, cnt_s, slot_s,
                hq, hx, msg, arr,
                v_s, meta_s, scol, dense, tal, hsum, hcount, quarters, parts, hquart, hparts,
                scaled, moved, place_s, poscol, slots_s, ssem, rsem, ysend, yrecv, hsend, hrecv, fsend, frecv, isem):
    gx, gy = lax.axis_index("gx"), lax.axis_index("gy")
    barrier = pltpu.get_barrier_semaphore()
    pairs = ((ks_in, ks_ref), (hk_in, hk_ref), (keys_in, keys_ref), (x_in, xin), (orders_in, orders_ref))
    inputs = [pltpu.make_async_copy(a, b, isem.at[i]) for i, (a, b) in enumerate(pairs)]
    for copy in inputs:
        copy.start()

    def greet(m, carry):
        for i in range(8):
            p = pair_at(gx, i // 2, offset(m)) + i % 2

            @pl.when(p != gx)
            def _():
                pl.semaphore_signal(barrier, inc=1, device_id={"gx": p}, device_id_type=MESH)

        return carry

    lax.fori_loop(0, 8, greet, 0)
    for k in range(1, GY):
        pl.semaphore_signal(barrier, inc=1, device_id={"gy": (gy + k) % GY}, device_id_type=MESH)

    chunks = xe.shape[0] // LANES
    hi_n, lo_n = 512, 256
    inputs[0].wait()
    inputs[1].wait()
    for i in range(2):
        ks = ks_ref[pl.ds(i, hi_n, stride=2), :]
        p1 = (ks >> 11) * 2 + ((ks >> 8) & 1)
        tab[i * W : (i + 1) * W, :] = p1.astype(F32).T.astype(BF16)
        tab[lo_n + i * W : lo_n + (i + 1) * W, :] = (ks & 255).astype(F32).T.astype(BF16)
    hk = jnp.concatenate([hk_ref[i : i + 1, :] for i in range(4)], axis=1)
    line = iota((16, hi_n), 0)
    digits = jnp.where(line == 0, hk & 255, jnp.where(line == 1, (hk >> 8) & 1, 0))
    digits = digits.astype(F32).astype(BF16)
    block = 2 * (iota((hi_n, hi_n), 1) >> 1)
    odd = (iota((1, hi_n), 1) & 1).astype(F32)
    marks = jnp.full((16, hi_n), -1.0, F32)
    for i in range(2):
        pick = jnp.where(iota((hi_n, hi_n), 0) == block + i, 1.0, 0.0).astype(BF16)
        found = dot(digits, pick)
        marks = jnp.where(line == i, jnp.where(found[1:2] == odd, found[0:1], -1.0), marks)
    tab[2 * lo_n : 2 * lo_n + 16, :] = marks.astype(BF16)
    z0, x0 = (gx // 2) % 8, gx // 16
    pt[...] = jnp.zeros_like(pt)

    def look(c, carry):
        block = keys_ref[pl.ds(pl.multiple_of(c * 8, 8), 8), :]
        key = jnp.concatenate([block[i : i + 1] for i in range(8)], axis=1)
        hi, lo = key >> 8, key & 255
        t = dot(tab[...], onehot(hi_n, LANES, 0, hi))
        mine = iota((lo_n, LANES), 0) == lo
        a = jnp.sum(jnp.where(mine, t[:lo_n], 0.0), axis=0, keepdims=True).astype(I32)
        b = jnp.sum(jnp.where(mine, t[lo_n : 2 * lo_n], 0.0), axis=0, keepdims=True).astype(I32)
        low = lo.astype(F32)
        second = t[2 * lo_n + 1 : 2 * lo_n + 2] == low
        heavy = (t[2 * lo_n : 2 * lo_n + 1] == low) | second
        owner = a >> 1
        dx = ((owner >> 4) + 4 - x0) & 3
        dz = (((owner >> 1) & 7) + 8 - z0) & 7
        zi = jnp.where(dz == 0, 0, jnp.where(dz <= 4, 2 * dz - 1, 16 - 2 * dz))
        place = (7 - zi) * 8 + dx * 2 + (owner & 1)
        shi = jnp.where(heavy, -1, owner * 8 + ((key >> 9) & 3) * 2 + (a & 1))
        shi_s[pl.ds(c, 1), :] = shi
        slo_s[pl.ds(c, 1), :] = b
        hid = (key >> 9) * 2 + jnp.where(second, 1, 0)
        seg_s[pl.ds(c, 1), :] = jnp.where(heavy, HALF + (hid & 255), (place >> 1) * CAPK)
        run_s[pl.ds(c, 1), :] = jnp.where(heavy, 2 * GX + (hid >> 5), (place >> 5) * CAPK)
        sub = jnp.where(heavy, hid, place) & 31
        line = iota((W, LANES), 0)
        kind = line >> 5
        facts = jnp.where(kind == 0, 1, jnp.where(kind == 1, b, jnp.where(kind == 2, shi & 7, 0)))
        facts = jnp.where((line & 31) == sub, facts, 0)
        at = pl.ds(pl.multiple_of(c * LANES, LANES), LANES)
        xm[at, :] = facts.astype(F32).T.astype(BF16)
        side = jnp.where(heavy, hid >> 8, place & 1).astype(F32)
        sides = jnp.broadcast_to(side, (W, LANES)).T.astype(BF16)
        x = xin[at, :]
        right = x * sides
        xe[at, 0:W] = x - right
        xe[at, W : 2 * W] = right
        pt[...] += dot_t(onehot(hi_n, LANES, 0, shi), onehot(lo_n, LANES, 0, b))
        return carry

    inputs[2].wait()
    inputs[3].wait()
    lax.fori_loop(0, chunks, look, 0, unroll=4)

    here = jnp.where(pt[...] > 0.5, 1.0, 0.0).T.astype(BF16)
    lower = jnp.where(iota((lo_n, lo_n), 1) < iota((lo_n, lo_n), 0), 1.0, 0.0).astype(BF16)
    r0, r1 = iota((hi_n, hi_n), 0), iota((hi_n, hi_n), 1)
    before = jnp.where((r0 < r1) & ((r0 >> 3) == (r1 >> 3)), 1.0, 0.0).astype(BF16)
    column = dot(jnp.ones((lo_n, lo_n), BF16), here).astype(BF16)
    rk[...] = (dot(lower, here) + dot(column, before)).astype(BF16)

    def rank(c, carry):
        shi = shi_s[pl.ds(c, 1), :]
        slo = slo_s[pl.ds(c, 1), :]
        t = dot(rk[...], onehot(hi_n, LANES, 0, shi))
        mine = iota((lo_n, LANES), 0) == slo
        r = jnp.sum(jnp.where(mine, t, 0.0), axis=0, keepdims=True).astype(I32)
        r = jnp.where(shi < 0, 0, r)
        seg_s[pl.ds(c, 1), :] = seg_s[pl.ds(c, 1), :] + r
        run_s[pl.ds(c, 1), :] = run_s[pl.ds(c, 1), :] + r
        return carry

    lax.fori_loop(0, chunks, rank, 0, unroll=4)

    def sums(base):
        total = None
        for c in range(chunks):
            at = slice(c * LANES, (c + 1) * LANES)
            part = dot(onehot(256, LANES, base, seg_s[c : c + 1, :]), xe[at, :])
            total = part if total is None else total + part
        return total

    ext[...] = jnp.zeros_like(ext)

    def gather_facts(c, carry):
        at = pl.ds(pl.multiple_of(c * LANES, LANES), LANES)
        ext[...] += dot(onehot(2 * GX + 16, LANES, 0, run_s[pl.ds(c, 1), :]), xm[at, :])
        return carry

    lax.fori_loop(0, chunks, gather_facts, 0, unroll=4)
    square = ext[0 : 2 * GX, :].T
    cnt = square[0:32]
    slot = jnp.floor((square[32:64] + 256.0 * square[64:96]) / jnp.maximum(cnt, 1.0) + 0.5)
    slot = jnp.where(cnt > 0.5, slot, -1.0)
    cnt_s[0:32, :] = cnt.astype(I32)
    cnt_s[32:64, :] = pltpu.roll(cnt, 64, 1).astype(I32)
    slot_s[0:32, :] = slot.astype(I32)
    slot_s[32:64, :] = pltpu.roll(slot, 64, 1).astype(I32)

    lane = iota((512, W), 1)
    counts = ext[2 * GX : 2 * GX + 16, :]
    high = jnp.floor(counts * (1.0 / 256.0))
    spread = jnp.where((iota((512, 16), 0) >> 5) == iota((512, 16), 1), 1.0, 0.0).astype(BF16)
    each = 256.0 * dot(spread, high.astype(BF16)) + dot(spread, (counts - 256.0 * high).astype(BF16))
    pick = lane == (iota((512, W), 0) & 31)
    counts = jnp.sum(jnp.where(pick, each, 0.0), axis=1, keepdims=True)

    def pack_heavy():
        both = acc[0]
        q, e = encode(jnp.concatenate([both[:, 0:W], both[:, W : 2 * W]], axis=0))
        hq[...] = q
        hx[...] = jnp.where(lane == 64, counts, jnp.where(lane == 65, e, 0.0)).astype(I32)

    acc[...] = jnp.zeros_like(acc)
    hq[...] = jnp.zeros_like(hq)
    hx[...] = jnp.zeros_like(hx)
    pl.semaphore_wait(barrier, GX + GY - 2)

    def to_owner(o):
        return pltpu.make_async_remote_copy(
            src_ref=msg.at[o], dst_ref=arr.at[gx], send_sem=ssem.at[o], recv_sem=rsem.at[gx],
            device_id={"gx": o}, device_id_type=MESH,
        )

    def send(m):
        for i in range(8):
            o = pair_at(gx, i // 2, offset(m)) + i % 2

            @pl.when(o != gx)
            def _():
                to_owner(o).start()

    def pack(m, both):
        q0, e0 = encode(both[:, 0:W])
        q1, e1 = encode(both[:, W : 2 * W])
        lane = iota((256, W), 1)
        e = jnp.where(lane == 0, e0, jnp.where(lane == 1, e1, 0.0)).T[0:8].astype(I32)
        pairs = [pair_at(gx, dx, offset(m)) for dx in range(4)]
        at = pl.ds(pl.multiple_of(m * 8, 8), 8)
        slots, counts = slot_s[at, :], cnt_s[at, :]
        lane, line = iota((8, W), 1), iota((8, W), 0)
        for i in range(8):
            o = pairs[i // 2] + i % 2
            part = e[i % 2 : i % 2 + 1, (i // 4) * W : (i // 4 + 1) * W]
            exps = pltpu.roll(part, 64, 1) if (i // 2) % 2 else part
            meta = jnp.where(line == 0, slots[i : i + 1], jnp.where(line == 1, counts[i : i + 1], exps))
            at = pl.ds(pl.multiple_of(o * 8, 8), 8)
            meta = jnp.where(lane < 64, meta, hx[at, :])
            values = (q1 if i % 2 else q0)[(i // 2) * 64 : (i // 2 + 1) * 64]
            msg[pl.ds(o, 1), 0:64, :] = values.astype(I16)[None]
            tail = jnp.concatenate([hq[at, :], meta], axis=0).astype(I16)
            msg[pl.ds(o, 1), 64:80, :] = tail[None]

    def owners(t, carry):
        @pl.when(t == 1)
        def _():
            pack_heavy()

        @pl.when(t == 2)
        def _():
            pack(0, acc[1])
            scol[0:KD, :] = slots_of(quarter_of(ks_ref, 0), gx)
            send(0)

        @pl.when(t > 3)
        def _():
            send(t - 3)

        pack(jnp.maximum(t - 2, 1), acc[pl.ds((t + 1) % 2, 1), :, :][0])
        acc[pl.ds(t % 2, 1), :, :] = sums(((t + 8) % 9) * 256)[None]
        return carry

    lax.fori_loop(0, 9, owners, 0)
    send(6)
    pack(7, acc[0])
    arr[pl.ds(gx, 1), :, :] = msg[pl.ds(gx, 1), :, :]

    for q in range(1, GY):
        at = slice(q * KD, (q + 1) * KD)
        scol[at, :] = slots_of(quarter_of(ks_ref, q), gx) + q * KD
    send(7)

    poscol[...] = slots_of(quarter_of(ks_ref, gy), gx)

    device = gx * GY + gy
    owners_here = [ks_ref[pl.ds(device * 4 + i, 1), :] >> 11 for i in range(4)]
    row = jnp.concatenate(owners_here, axis=1)
    square = jnp.zeros((W, W), I32)
    for i in range(4):
        square = jnp.where(iota((W, W), 0) == i, owners_here[i], square)
    square = square.astype(F32).T.astype(I32)
    col = jnp.concatenate([square[:, i : i + 1] for i in range(4)], axis=0)
    j0, j1 = iota((KD, KD), 0), iota((KD, KD), 1)
    w = jnp.sum(jnp.where((row == col) & (j1 < j0), 1.0, 0.0), axis=1, keepdims=True)
    place_s[...] = jnp.where(col * 8 + w.astype(I32) == j1, 1.0, 0.0).astype(BF16)

    dense[...] = jnp.zeros_like(dense)
    tal[...] = jnp.zeros_like(tal)
    hsum[...] = jnp.zeros_like(hsum)
    hcount[...] = jnp.zeros_like(hcount)
    lane8 = iota((8, W), 1)

    def arrive(m, carry):
        def wait(i, carry):
            s = pair_at(gx, -(i // 2), -offset(m)) + i % 2

            @pl.when(s != gx)
            def _():
                pltpu.make_async_remote_copy(
                    src_ref=msg.at[s], dst_ref=arr.at[s], send_sem=ssem.at[s],
                    recv_sem=rsem.at[s], device_id={"gx": s}, device_id_type=MESH,
                ).wait_recv()

            return carry

        lax.fori_loop(0, 8, wait, 0)
        for dx in range(4):
            pair = pair_at(gx, -dx, -offset(m))
            metas = []
            for i in range(2):
                s = pair + i

                q = arr[pl.ds(s, 1), 0:64, :][0].astype(I32)
                high = q >> 8
                at = slice((dx * 2 + i) * 64, (dx * 2 + i + 1) * 64)
                v_s[at, 0:W] = high.astype(F32).astype(BF16)
                v_s[at, W : 2 * W] = (q - high * 256).astype(F32).astype(BF16)
                tail = arr[pl.ds(s, 1), 64:80, :][0].astype(I32)
                meta = tail[8:16]
                hsum[...] += tail[0:8].astype(F32) * power(meta[:, 65:66].astype(F32))
                hcount[...] += meta[:, 64:65].astype(F32) + jnp.zeros((8, W), F32)
                metas.append(meta)
            meta_s[:, dx * W : (dx + 1) * W] = jnp.where(
                lane8 < 64, metas[0], pltpu.roll(metas[1], 64, 1)
            )
        meta = meta_s[...]
        scale = power(meta[2:3].astype(F32))
        count = meta[1:2].astype(F32)

        for q in range(GY):
            at = slice(q * KD, (q + 1) * KD)
            mine = scol[at, :] == meta[0:1]
            dense[at, :] += dot(jnp.where(mine, scale, 0.0).astype(BF16), v_s[...])
            hits = jnp.where(mine, count, 0.0)
            tal[at, :] += (hits[:, 0:W] + hits[:, W : 2 * W]) + (
                hits[:, 2 * W : 3 * W] + hits[:, 3 * W : 4 * W]
            )
        return carry

    lax.fori_loop(0, 8, arrive, 0)

    line8 = iota((8, W), 0)
    for q in range(GY):
        rows = jnp.where(line8 == 0, hsum[2 * q : 2 * q + 1], 0.0)
        rows = jnp.where(line8 == 1, hsum[2 * q + 1 : 2 * q + 2], rows)
        rows = jnp.where(line8 == 2, hcount[2 * q : 2 * q + 1], rows)
        rows = jnp.where(line8 == 3, hcount[2 * q + 1 : 2 * q + 2], rows)
        hquart[q, :, :] = rows

    def to_quarter(h, p):
        return pltpu.make_async_remote_copy(
            src_ref=quarters.at[h * GY + p], dst_ref=parts.at[h * GY + gy],
            send_sem=ysend.at[h * GY + p], recv_sem=yrecv.at[h * GY + gy],
            device_id={"gy": p}, device_id_type=MESH,
        )

    def heavy_to(p):
        return pltpu.make_async_remote_copy(
            src_ref=hquart.at[p], dst_ref=hparts.at[gy], send_sem=hsend.at[p],
            recv_sem=hrecv.at[gy], device_id={"gy": p}, device_id_type=MESH,
        )

    def piece_at(n):
        return n // (GY - 1), (gy + n % (GY - 1) + 1) % GY

    def leave(n, carry):
        @pl.when(n > 0)
        def _():
            to_quarter(*piece_at(n - 1)).start()

        h, p = piece_at(n)
        at = pl.ds(pl.multiple_of(p * KD + h * HK, HK), HK)
        q, e = encode(dense[at, 0:W] * 256.0 + dense[at, W : 2 * W])
        q = q.astype(I16)
        t = jnp.sum(tal[at, :].T, axis=0, keepdims=True)
        e = jnp.where(iota((HK, W), 1) == 0, e, 0.0).T[0:1]
        line = iota((16, W), 0)
        rows = jnp.zeros((16, W), F32)
        rows = jnp.where(line == 0, t, jnp.where(line == 1, e, rows))
        rows = rows.astype(I32).astype(I16)
        quarters[pl.ds(h * GY + p, 1), 0:HK, :] = q[None]
        quarters[pl.ds(h * GY + p, 1), HK : HK + 16, :] = rows[None]
        return carry

    lax.fori_loop(0, NP * (GY - 1), leave, 0)
    for k in range(1, GY):
        heavy_to((gy + k) % GY).start()
    to_quarter(*piece_at(NP * (GY - 1) - 1)).start()
    def to_range(k, p):
        return pltpu.make_async_remote_copy(
            src_ref=scaled.at[k], dst_ref=moved.at[gx], send_sem=fsend.at[p],
            recv_sem=frecv.at[gx], device_id={"gx": p}, device_id_type=MESH,
        )

    slots_s[...] = jnp.zeros_like(slots_s)

    def piece(h, carry):
        at = pl.ds(pl.multiple_of(gy * KD + h * HK, HK), HK)
        total = dense[at, 0:W] * 256.0 + dense[at, W : 2 * W]
        col = jnp.sum(tal[at, :], axis=1, keepdims=True)
        for k in range(1, GY):
            s = (gy + GY - k) % GY
            pltpu.make_async_remote_copy(
                src_ref=quarters.at[h * GY + s], dst_ref=parts.at[h * GY + s],
                send_sem=ysend.at[h * GY + s], recv_sem=yrecv.at[h * GY + s],
                device_id={"gy": s}, device_id_type=MESH,
            ).wait_recv()
        for k in range(1, GY):
            s = (gy + GY - k) % GY
            rows = parts[pl.ds(h * GY + s, 1), HK : HK + 16, :][0].astype(F32)
            square = jnp.concatenate([rows, jnp.zeros((W - 16, W), F32)], axis=0).T
            scale = square[:, 1:2]
            total = total + parts[pl.ds(h * GY + s, 1), 0:HK, :][0].astype(F32) * power(scale)
            col = col + square[:, 0:1]
        at = pl.ds(h * (GX // NP), GX // NP)
        scaled[at, :, :] = (total * lax.rsqrt(1.0 + col)).reshape(GX // NP, 8, W)
        pos = poscol[pl.ds(pl.multiple_of(h * HK, HK), HK), :]
        slots_s[...] += jnp.sum(
            jnp.where(pos == iota((HK, KD), 1), col, 0.0), axis=0, keepdims=True
        )

        def range_out(m, carry):
            for i in range(8):
                p = pair_at(gx, i // 2, offset(m)) + i % 2

                @pl.when(p != gx)
                def _():
                    to_range(m * 8 + i, p).start()

            return carry

        lax.fori_loop(h * (8 // NP), (h + 1) * (8 // NP), range_out, 0)
        return carry

    lax.fori_loop(0, NP, piece, 0)
    moved[pl.ds(gx, 1), :, :] = scaled[pl.ds(56 + gx % 2, 1), :, :]
    slots = slots_s[...]
    slots_ref[...] = jnp.concatenate([slots[:, i * W : (i + 1) * W] for i in range(4)], axis=0)
    tail = hquart[pl.ds(gy, 1), :, :][0]
    for k in range(1, GY):
        s = (gy + GY - k) % GY
        pltpu.make_async_remote_copy(
            src_ref=hquart.at[s], dst_ref=hparts.at[s], send_sem=hsend.at[s],
            recv_sem=hrecv.at[s], device_id={"gy": s}, device_id_type=MESH,
        ).wait_recv()
        tail = tail + hparts[pl.ds(s, 1), :, :][0]

    def finish(k, carry):
        s = (gx + k) % GX
        to_owner(s).wait_send()
        to_range(s, s).wait_send()
        pltpu.make_async_remote_copy(
            src_ref=scaled.at[s], dst_ref=moved.at[s], send_sem=fsend.at[s],
            recv_sem=frecv.at[s], device_id={"gx": s}, device_id_type=MESH,
        ).wait_recv()
        return carry

    lax.fori_loop(1, GX, finish, 0)
    for k in range(1, GY):
        for h in range(NP):
            to_quarter(h, (gy + k) % GY).wait_send()
        heavy_to((gy + k) % GY).wait_send()

    inputs[4].wait()
    got = moved[...].reshape(KD, W)
    high = got.astype(BF16)
    low = (got - high.astype(F32)).astype(BF16)
    both = dot(place_s[...], jnp.concatenate([high, low], axis=1))
    total = both[:, 0:W] + both[:, W : 2 * W]
    orders = orders_ref[...].astype(F32)
    heavy = tail * lax.rsqrt(1.0 + pltpu.roll(tail, 6, 0))
    line = iota((KD, W), 0)
    reports = []
    for h in range(2):
        ours = iota((1, KD), 1) == 2 * device + h
        key = jnp.sum(jnp.where(ours, hk, 0).astype(F32), axis=1, keepdims=True).astype(I32)
        here = line == key - device * KD
        total = jnp.where(here, heavy[h : h + 1, :], total)
        mine = jnp.sum(jnp.where(here, orders, 0.0), axis=0, keepdims=True)
        reports.append(mine * heavy[h : h + 1, :])
    out_ref[...] = (orders * total).astype(BF16)
    report_ref[...] = jnp.concatenate(reports, axis=0).astype(BF16)


def join(keys, x, ks, heavy_keys, orders):
    rows = x.shape[0]
    chunks = rows // LANES
    dma = pltpu.SemaphoreType.DMA
    return pl.pallas_call(
        join_kernel,
        out_shape=(
            jax.ShapeDtypeStruct((KD, W), BF16),
            jax.ShapeDtypeStruct((2, W), BF16),
            jax.ShapeDtypeStruct((4, W), F32),
        ),
        in_specs=[pl.BlockSpec(memory_space=pl.ANY)] * 5,
        out_specs=(VMEM,) * 3,
        scratch_shapes=[
            pltpu.VMEM(keys.shape, I32),
            pltpu.VMEM(ks.shape, I32),
            pltpu.VMEM(heavy_keys.shape, I32),
            pltpu.VMEM(orders.shape, BF16),
            pltpu.VMEM((528, 512), BF16),
            pltpu.VMEM((chunks, LANES), I32),
            pltpu.VMEM((chunks, LANES), I32),
            pltpu.VMEM((chunks, LANES), I32),
            pltpu.VMEM((chunks, LANES), I32),
            pltpu.VMEM((rows, W), BF16),
            pltpu.VMEM((rows, W), BF16),
            pltpu.VMEM((rows, 2 * W), BF16),
            pltpu.VMEM((512, 256), F32),
            pltpu.VMEM((256, 512), BF16),
            pltpu.VMEM((2, 256, 2 * W), F32),
            pltpu.VMEM((2 * GX + 16, W), F32),
            pltpu.VMEM((GX, W), I32),
            pltpu.VMEM((GX, W), I32),
            pltpu.VMEM((512, W), I32),
            pltpu.VMEM((512, W), I32),
            pltpu.VMEM((GX, MSG, W), I16),
            pltpu.VMEM((GX, MSG, W), I16),
            pltpu.VMEM((512, 2 * W), BF16),
            pltpu.VMEM((8, 512), I32),
            pltpu.VMEM((OWN, 1), I32),
            pltpu.VMEM((OWN, 2 * W), F32),
            pltpu.VMEM((OWN, W), F32),
            pltpu.VMEM((8, W), F32),
            pltpu.VMEM((8, W), F32),
            pltpu.VMEM((NP * GY, HK + 16, W), I16),
            pltpu.VMEM((NP * GY, HK + 16, W), I16),
            pltpu.VMEM((GY, 8, W), F32),
            pltpu.VMEM((GY, 8, W), F32),
            pltpu.VMEM((GX, 8, W), F32),
            pltpu.VMEM((GX, 8, W), F32),
            pltpu.VMEM((KD, KD), BF16),
            pltpu.VMEM((KD, 1), I32),
            pltpu.VMEM((1, KD), F32),
            dma((GX,)), dma((GX,)), dma((NP * GY,)), dma((NP * GY,)), dma((GY,)), dma((GY,)),
            dma((GX,)), dma((GX,)), dma((5,)),
        ],
        compiler_params=pltpu.CompilerParams(
            collective_id=0, has_side_effects=True, vmem_limit_bytes=56 * 2**20
        ),
        name="join_rows",
    )(keys, x, ks, heavy_keys, orders)


def hand_on_kernel(a_ref, b_ref, c_ref, out_a, out_b, out_c):
    out_a[...] = a_ref[...]
    out_b[...] = b_ref[...]
    out_c[...] = c_ref[...]


def hand_on(*arrays):
    return pl.pallas_call(
        hand_on_kernel,
        out_shape=tuple(jax.ShapeDtypeStruct(a.shape, a.dtype) for a in arrays),
        in_specs=[VMEM] * 3,
        out_specs=(VMEM,) * 3,
        name="hand_on",
    )(*arrays)


def body(measures, row_keys, orders, heavy_keys, key_slot):
    result, report, slot_rows = join(
        row_keys.reshape(-1, W), measures, key_slot.reshape(-1, W), heavy_keys.reshape(-1, W), orders
    )
    result, report, slot_rows = hand_on(result, report, slot_rows)
    return (result, report, slot_rows.reshape(KD))


def solution(mesh):
    return jax.shard_map(
        body,
        mesh=mesh,
        in_specs=(P(("gx", "gy"), None), P(("gx", "gy")), P(("gx", "gy"), None), P(), P()),
        out_specs=(P(("gx", "gy"), None), P(("gx", "gy"), None), P(("gx", "gy"))),
        check_vma=False,
    )
```

```python
import jax
import jax.numpy as jnp
from jax import lax
from jax.experimental import pallas as pl
from jax.experimental.pallas import tpu as pltpu
from jax.sharding import PartitionSpec as P

MESH = pl.DeviceIdType.MESH
F32, BF16, I32, I16 = jnp.float32, jnp.bfloat16, jnp.int32, jnp.int16
LN2 = 0.6931471805599453

W = 128
GX, GY = 64, 4
KEYS = 131072
KD = 512
HK = 128
NP = KD // HK
OWN = 2048
CAPK = 64
HALF = 2048
HG = 8
MSG = 80
LANES = 1024
VMEM = pl.BlockSpec(memory_space=pltpu.VMEM)


def iota(shape, dim):
    return lax.broadcasted_iota(I32, shape, dim)


def onehot(rows, lanes, base, labels):
    labels = (labels - base).astype(I16)
    return jnp.where(iota((rows, lanes), 0).astype(I16) == labels, jnp.ones((), BF16), jnp.zeros((), BF16))


def dot(a, b):
    return jnp.dot(a, b, preferred_element_type=F32)


def dot_t(a, b):
    return lax.dot_general(a, b, (((1,), (1,)), ((), ())), preferred_element_type=F32)


def power(e):
    return jnp.exp(e * LN2)


def encode(v):
    top = jnp.max(jnp.abs(v), axis=1, keepdims=True)
    e = jnp.ceil(jnp.log(jnp.maximum(top, 1e-30)) * (1.0 / LN2) - 14.99)
    e = jnp.maximum(e, -100.0)
    q = jnp.floor(v * power(-e) + 0.5).astype(I32)
    return q, e


def quarter_of(ks_ref, q):
    rows = [ks_ref[pl.ds(q * 4 + i, GX, stride=16), :] for i in range(4)]
    return jnp.concatenate(rows, axis=1)


def slots_of(ks, me):
    mine = jnp.where((ks >> 11) == me, 1.0, 0.0)
    upper = jnp.where(iota((KD, KD), 0) < iota((KD, KD), 1), 1.0, 0.0).astype(BF16)
    w = dot(mine.astype(BF16), upper)
    pos = (ks & (KD - 1)).astype(F32)
    lane = iota((GX, W), 1)
    table = jnp.zeros((GX, W), F32)
    for k in range(8):
        s = jnp.sum(jnp.where((mine > 0.5) & (w == float(k)), pos, 0.0), axis=1, keepdims=True)
        table = jnp.where(lane == k, s, table)
    high = jnp.floor(table * (1.0 / 256.0))
    low = table - 256.0 * high
    place = iota((KD, GX), 0) >> 3
    zi = 7 - (place >> 3)
    dz = ((zi + 1) >> 1) * (1 - 2 * ((zi + 1) & 1))
    z, x = (me // 2) % 8 + 8 + dz, me // 16 + ((place >> 1) & 3)
    block = ((x & 3) * 8 + (z & 7)) * 2 + (place & 1)
    repeat = jnp.where(block == iota((KD, GX), 1), 1.0, 0.0).astype(BF16)
    each = 256.0 * dot(repeat, high.astype(BF16)) + dot(repeat, low.astype(BF16))
    pick = iota((KD, W), 1) == (iota((KD, W), 0) & 7)
    return jnp.sum(jnp.where(pick, each, 0.0), axis=1, keepdims=True).astype(I32)


def offset(m):
    zi = 7 - m
    return ((zi + 1) // 2) * (1 - 2 * ((zi + 1) % 2))


def pair_at(me, dx, dz):
    z, x = (me // 2) % 8, me // 16
    return (((x + 4 + dx) % 4) * 8 + (z + 8 + dz) % 8) * 2


def join_kernel(keys_in, x_in, ks_in, hk_in, orders_in,
                out_ref, report_ref, slots_ref,
                keys_ref, ks_ref, hk_ref, orders_ref, tab, shi_s, slo_s, seg_s, run_s, xin, xm, xe, pt, rk, acc, ext, cnt_s, slot_s,
                hq, hx, msg, arr,
                v_s, meta_s, scol, dense, tal, hsum, hcount, quarters, parts, hquart, hparts,
                scaled, moved, place_s, poscol, slots_s, ssem, rsem, ysend, yrecv, hsend, hrecv, fsend, frecv, isem):
    gx, gy = lax.axis_index("gx"), lax.axis_index("gy")
    barrier = pltpu.get_barrier_semaphore()
    pairs = ((ks_in, ks_ref), (hk_in, hk_ref), (keys_in, keys_ref), (x_in, xin), (orders_in, orders_ref))
    inputs = [pltpu.make_async_copy(a, b, isem.at[i]) for i, (a, b) in enumerate(pairs)]
    for copy in inputs:
        copy.start()

    def greet(m, carry):
        for i in range(8):
            p = pair_at(gx, i // 2, offset(m)) + i % 2

            @pl.when(p != gx)
            def _():
                pl.semaphore_signal(barrier, inc=1, device_id={"gx": p}, device_id_type=MESH)

        return carry

    lax.fori_loop(0, 8, greet, 0)
    for k in range(1, GY):
        pl.semaphore_signal(barrier, inc=1, device_id={"gy": (gy + k) % GY}, device_id_type=MESH)

    chunks = xe.shape[0] // LANES
    hi_n, lo_n = 512, 256
    inputs[0].wait()
    inputs[1].wait()
    for i in range(2):
        ks = ks_ref[pl.ds(i, hi_n, stride=2), :]
        p1 = (ks >> 11) * 2 + ((ks >> 8) & 1)
        tab[i * W : (i + 1) * W, :] = p1.astype(F32).T.astype(BF16)
        tab[lo_n + i * W : lo_n + (i + 1) * W, :] = (ks & 255).astype(F32).T.astype(BF16)
    hk = jnp.concatenate([hk_ref[i : i + 1, :] for i in range(4)], axis=1)
    line = iota((16, hi_n), 0)
    digits = jnp.where(line == 0, hk & 255, jnp.where(line == 1, (hk >> 8) & 1, 0))
    digits = digits.astype(F32).astype(BF16)
    block = 2 * (iota((hi_n, hi_n), 1) >> 1)
    odd = (iota((1, hi_n), 1) & 1).astype(F32)
    marks = jnp.full((16, hi_n), -1.0, F32)
    for i in range(2):
        pick = jnp.where(iota((hi_n, hi_n), 0) == block + i, 1.0, 0.0).astype(BF16)
        found = dot(digits, pick)
        marks = jnp.where(line == i, jnp.where(found[1:2] == odd, found[0:1], -1.0), marks)
    tab[2 * lo_n : 2 * lo_n + 16, :] = marks.astype(BF16)
    z0, x0 = (gx // 2) % 8, gx // 16
    pt[...] = jnp.zeros_like(pt)

    def look(c, carry):
        block = keys_ref[pl.ds(pl.multiple_of(c * 8, 8), 8), :]
        key = jnp.concatenate([block[i : i + 1] for i in range(8)], axis=1)
        hi, lo = key >> 8, key & 255
        t = dot(tab[...], onehot(hi_n, LANES, 0, hi))
        mine = iota((lo_n, LANES), 0) == lo
        a = jnp.sum(jnp.where(mine, t[:lo_n], 0.0), axis=0, keepdims=True).astype(I32)
        b = jnp.sum(jnp.where(mine, t[lo_n : 2 * lo_n], 0.0), axis=0, keepdims=True).astype(I32)
        low = lo.astype(F32)
        second = t[2 * lo_n + 1 : 2 * lo_n + 2] == low
        heavy = (t[2 * lo_n : 2 * lo_n + 1] == low) | second
        owner = a >> 1
        dx = ((owner >> 4) + 4 - x0) & 3
        dz = (((owner >> 1) & 7) + 8 - z0) & 7
        zi = jnp.where(dz == 0, 0, jnp.where(dz <= 4, 2 * dz - 1, 16 - 2 * dz))
        place = (7 - zi) * 8 + dx * 2 + (owner & 1)
        shi = jnp.where(heavy, -1, owner * 8 + ((key >> 9) & 3) * 2 + (a & 1))
        shi_s[pl.ds(c, 1), :] = shi
        slo_s[pl.ds(c, 1), :] = b
        hid = (key >> 9) * 2 + jnp.where(second, 1, 0)
        seg_s[pl.ds(c, 1), :] = jnp.where(heavy, HALF + (hid & 255), (place >> 1) * CAPK)
        run_s[pl.ds(c, 1), :] = jnp.where(heavy, 2 * GX + (hid >> 5), (place >> 5) * CAPK)
        sub = jnp.where(heavy, hid, place) & 31
        line = iota((W, LANES), 0)
        kind = line >> 5
        facts = jnp.where(kind == 0, 1, jnp.where(kind == 1, b, jnp.where(kind == 2, shi & 7, 0)))
        facts = jnp.where((line & 31) == sub, facts, 0)
        at = pl.ds(pl.multiple_of(c * LANES, LANES), LANES)
        xm[at, :] = facts.astype(F32).T.astype(BF16)
        side = jnp.where(heavy, hid >> 8, place & 1).astype(F32)
        sides = jnp.broadcast_to(side, (W, LANES)).T.astype(BF16)
        x = xin[at, :]
        right = x * sides
        xe[at, 0:W] = x - right
        xe[at, W : 2 * W] = right
        pt[...] += dot_t(onehot(hi_n, LANES, 0, shi), onehot(lo_n, LANES, 0, b))
        return carry

    inputs[2].wait()
    inputs[3].wait()
    lax.fori_loop(0, chunks, look, 0, unroll=4)

    here = jnp.where(pt[...] > 0.5, 1.0, 0.0).T.astype(BF16)
    lower = jnp.where(iota((lo_n, lo_n), 1) < iota((lo_n, lo_n), 0), 1.0, 0.0).astype(BF16)
    r0, r1 = iota((hi_n, hi_n), 0), iota((hi_n, hi_n), 1)
    before = jnp.where((r0 < r1) & ((r0 >> 3) == (r1 >> 3)), 1.0, 0.0).astype(BF16)
    column = dot(jnp.ones((lo_n, lo_n), BF16), here).astype(BF16)
    rk[...] = (dot(lower, here) + dot(column, before)).astype(BF16)

    def rank(c, carry):
        shi = shi_s[pl.ds(c, 1), :]
        slo = slo_s[pl.ds(c, 1), :]
        t = dot(rk[...], onehot(hi_n, LANES, 0, shi))
        mine = iota((lo_n, LANES), 0) == slo
        r = jnp.sum(jnp.where(mine, t, 0.0), axis=0, keepdims=True).astype(I32)
        r = jnp.where(shi < 0, 0, r)
        seg_s[pl.ds(c, 1), :] = seg_s[pl.ds(c, 1), :] + r
        run_s[pl.ds(c, 1), :] = run_s[pl.ds(c, 1), :] + r
        return carry

    lax.fori_loop(0, chunks, rank, 0, unroll=4)

    def sums(base):
        total = None
        for c in range(chunks):
            at = slice(c * LANES, (c + 1) * LANES)
            part = dot(onehot(256, LANES, base, seg_s[c : c + 1, :]), xe[at, :])
            total = part if total is None else total + part
        return total

    ext[...] = jnp.zeros_like(ext)

    def gather_facts(c, carry):
        at = pl.ds(pl.multiple_of(c * LANES, LANES), LANES)
        ext[...] += dot(onehot(2 * GX + 16, LANES, 0, run_s[pl.ds(c, 1), :]), xm[at, :])
        return carry

    lax.fori_loop(0, chunks, gather_facts, 0, unroll=4)
    square = ext[0 : 2 * GX, :].T
    cnt = square[0:32]
    slot = jnp.floor((square[32:64] + 256.0 * square[64:96]) / jnp.maximum(cnt, 1.0) + 0.5)
    slot = jnp.where(cnt > 0.5, slot, -1.0)
    cnt_s[0:32, :] = cnt.astype(I32)
    cnt_s[32:64, :] = pltpu.roll(cnt, 64, 1).astype(I32)
    slot_s[0:32, :] = slot.astype(I32)
    slot_s[32:64, :] = pltpu.roll(slot, 64, 1).astype(I32)

    lane = iota((512, W), 1)
    counts = ext[2 * GX : 2 * GX + 16, :]
    high = jnp.floor(counts * (1.0 / 256.0))
    spread = jnp.where((iota((512, 16), 0) >> 5) == iota((512, 16), 1), 1.0, 0.0).astype(BF16)
    each = 256.0 * dot(spread, high.astype(BF16)) + dot(spread, (counts - 256.0 * high).astype(BF16))
    pick = lane == (iota((512, W), 0) & 31)
    counts = jnp.sum(jnp.where(pick, each, 0.0), axis=1, keepdims=True)

    def pack_heavy():
        both = acc[0]
        q, e = encode(jnp.concatenate([both[:, 0:W], both[:, W : 2 * W]], axis=0))
        hq[...] = q
        hx[...] = jnp.where(lane == 64, counts, jnp.where(lane == 65, e, 0.0)).astype(I32)

    acc[...] = jnp.zeros_like(acc)
    hq[...] = jnp.zeros_like(hq)
    hx[...] = jnp.zeros_like(hx)
    pl.semaphore_wait(barrier, GX + GY - 2)

    def to_owner(o):
        return pltpu.make_async_remote_copy(
            src_ref=msg.at[o], dst_ref=arr.at[gx], send_sem=ssem.at[o], recv_sem=rsem.at[gx],
            device_id={"gx": o}, device_id_type=MESH,
        )

    def send(m):
        for i in range(8):
            o = pair_at(gx, i // 2, offset(m)) + i % 2

            @pl.when(o != gx)
            def _():
                to_owner(o).start()

    def pack(m, both):
        q0, e0 = encode(both[:, 0:W])
        q1, e1 = encode(both[:, W : 2 * W])
        lane = iota((256, W), 1)
        e = jnp.where(lane == 0, e0, jnp.where(lane == 1, e1, 0.0)).T[0:8].astype(I32)
        pairs = [pair_at(gx, dx, offset(m)) for dx in range(4)]
        at = pl.ds(pl.multiple_of(m * 8, 8), 8)
        slots, counts = slot_s[at, :], cnt_s[at, :]
        lane, line = iota((8, W), 1), iota((8, W), 0)
        for i in range(8):
            o = pairs[i // 2] + i % 2
            part = e[i % 2 : i % 2 + 1, (i // 4) * W : (i // 4 + 1) * W]
            exps = pltpu.roll(part, 64, 1) if (i // 2) % 2 else part
            meta = jnp.where(line == 0, slots[i : i + 1], jnp.where(line == 1, counts[i : i + 1], exps))
            at = pl.ds(pl.multiple_of(o * 8, 8), 8)
            meta = jnp.where(lane < 64, meta, hx[at, :])
            values = (q1 if i % 2 else q0)[(i // 2) * 64 : (i // 2 + 1) * 64]
            msg[pl.ds(o, 1), 0:64, :] = values.astype(I16)[None]
            tail = jnp.concatenate([hq[at, :], meta], axis=0).astype(I16)
            msg[pl.ds(o, 1), 64:80, :] = tail[None]

    def owners(t, carry):
        @pl.when(t == 1)
        def _():
            pack_heavy()

        @pl.when(t == 2)
        def _():
            pack(0, acc[1])
            scol[0:KD, :] = slots_of(quarter_of(ks_ref, 0), gx)
            send(0)

        @pl.when(t > 3)
        def _():
            send(t - 3)

        pack(jnp.maximum(t - 2, 1), acc[pl.ds((t + 1) % 2, 1), :, :][0])
        acc[pl.ds(t % 2, 1), :, :] = sums(((t + 8) % 9) * 256)[None]
        return carry

    lax.fori_loop(0, 9, owners, 0)
    send(6)
    pack(7, acc[0])
    arr[pl.ds(gx, 1), :, :] = msg[pl.ds(gx, 1), :, :]

    for q in range(1, GY):
        at = slice(q * KD, (q + 1) * KD)
        scol[at, :] = slots_of(quarter_of(ks_ref, q), gx) + q * KD
    send(7)

    dense[...] = jnp.zeros_like(dense)
    tal[...] = jnp.zeros_like(tal)
    hsum[...] = jnp.zeros_like(hsum)
    hcount[...] = jnp.zeros_like(hcount)
    lane8 = iota((8, W), 1)

    def arrive(m, carry):
        def wait(i, carry):
            s = pair_at(gx, -(i // 2), -offset(m)) + i % 2

            @pl.when(s != gx)
            def _():
                pltpu.make_async_remote_copy(
                    src_ref=msg.at[s], dst_ref=arr.at[s], send_sem=ssem.at[s],
                    recv_sem=rsem.at[s], device_id={"gx": s}, device_id_type=MESH,
                ).wait_recv()

            return carry

        lax.fori_loop(0, 8, wait, 0)
        for dx in range(4):
            pair = pair_at(gx, -dx, -offset(m))
            metas = []
            for i in range(2):
                s = pair + i

                q = arr[pl.ds(s, 1), 0:64, :][0].astype(I32)
                high = q >> 8
                at = slice((dx * 2 + i) * 64, (dx * 2 + i + 1) * 64)
                v_s[at, 0:W] = high.astype(F32).astype(BF16)
                v_s[at, W : 2 * W] = (q - high * 256).astype(F32).astype(BF16)
                tail = arr[pl.ds(s, 1), 64:80, :][0].astype(I32)
                meta = tail[8:16]
                hsum[...] += tail[0:8].astype(F32) * power(meta[:, 65:66].astype(F32))
                hcount[...] += meta[:, 64:65].astype(F32) + jnp.zeros((8, W), F32)
                metas.append(meta)
            meta_s[:, dx * W : (dx + 1) * W] = jnp.where(
                lane8 < 64, metas[0], pltpu.roll(metas[1], 64, 1)
            )
        meta = meta_s[...]
        scale = power(meta[2:3].astype(F32))
        count = meta[1:2].astype(F32)

        for q in range(GY):
            at = slice(q * KD, (q + 1) * KD)
            mine = scol[at, :] == meta[0:1]
            dense[at, :] += dot(jnp.where(mine, scale, 0.0).astype(BF16), v_s[...])
            hits = jnp.where(mine, count, 0.0)
            tal[at, :] += (hits[:, 0:W] + hits[:, W : 2 * W]) + (
                hits[:, 2 * W : 3 * W] + hits[:, 3 * W : 4 * W]
            )
        return carry

    lax.fori_loop(0, 8, arrive, 0)

    line8 = iota((8, W), 0)
    for q in range(GY):
        rows = jnp.where(line8 == 0, hsum[2 * q : 2 * q + 1], 0.0)
        rows = jnp.where(line8 == 1, hsum[2 * q + 1 : 2 * q + 2], rows)
        rows = jnp.where(line8 == 2, hcount[2 * q : 2 * q + 1], rows)
        rows = jnp.where(line8 == 3, hcount[2 * q + 1 : 2 * q + 2], rows)
        hquart[q, :, :] = rows

    def to_quarter(h, p):
        return pltpu.make_async_remote_copy(
            src_ref=quarters.at[h * GY + p], dst_ref=parts.at[h * GY + gy],
            send_sem=ysend.at[h * GY + p], recv_sem=yrecv.at[h * GY + gy],
            device_id={"gy": p}, device_id_type=MESH,
        )

    def heavy_to(p):
        return pltpu.make_async_remote_copy(
            src_ref=hquart.at[p], dst_ref=hparts.at[gy], send_sem=hsend.at[p],
            recv_sem=hrecv.at[gy], device_id={"gy": p}, device_id_type=MESH,
        )

    def leave(n, carry):
        h, k = n // GY, n % GY + 1
        p = (gy + k) % GY
        at = pl.ds(pl.multiple_of(p * KD + h * HK, HK), HK)
        q, e = encode(dense[at, 0:W] * 256.0 + dense[at, W : 2 * W])
        q = q.astype(I16)
        t = jnp.sum(tal[at, :].T, axis=0, keepdims=True)
        e = jnp.where(iota((HK, W), 1) == 0, e, 0.0).T[0:1]
        line = iota((16, W), 0)
        rows = jnp.zeros((16, W), F32)
        rows = jnp.where(line == 0, t, jnp.where(line == 1, e, rows))
        rows = rows.astype(I32).astype(I16)
        quarters[pl.ds(h * GY + p, 1), 0:HK, :] = q[None]
        quarters[pl.ds(h * GY + p, 1), HK : HK + 16, :] = rows[None]

        @pl.when(k > 1)
        def _():
            to_quarter(h, (gy + k - 1) % GY).start()

        @pl.when(k == GY)
        def _():
            parts[pl.ds(h * GY + gy, 1), 0:HK, :] = q[None]
            parts[pl.ds(h * GY + gy, 1), HK : HK + 16, :] = rows[None]

        return carry

    lax.fori_loop(0, NP * GY, leave, 0)
    for k in range(1, GY):
        heavy_to((gy + k) % GY).start()
    poscol[...] = slots_of(quarter_of(ks_ref, gy), gx)

    device = gx * GY + gy
    owners_here = [ks_ref[pl.ds(device * 4 + i, 1), :] >> 11 for i in range(4)]
    row = jnp.concatenate(owners_here, axis=1)
    square = jnp.zeros((W, W), I32)
    for i in range(4):
        square = jnp.where(iota((W, W), 0) == i, owners_here[i], square)
    square = square.astype(F32).T.astype(I32)
    col = jnp.concatenate([square[:, i : i + 1] for i in range(4)], axis=0)
    j0, j1 = iota((KD, KD), 0), iota((KD, KD), 1)
    w = jnp.sum(jnp.where((row == col) & (j1 < j0), 1.0, 0.0), axis=1, keepdims=True)
    place_s[...] = jnp.where(col * 8 + w.astype(I32) == j1, 1.0, 0.0).astype(BF16)

    def to_range(k, p):
        return pltpu.make_async_remote_copy(
            src_ref=scaled.at[k], dst_ref=moved.at[gx], send_sem=fsend.at[p],
            recv_sem=frecv.at[gx], device_id={"gx": p}, device_id_type=MESH,
        )

    slots_s[...] = jnp.zeros_like(slots_s)

    def piece(h, carry):
        total, tallies = jnp.zeros((HK, W), F32), jnp.zeros((W, W), F32)
        for k in range(1, GY):
            s = (gy + GY - k) % GY
            pltpu.make_async_remote_copy(
                src_ref=quarters.at[h * GY + s], dst_ref=parts.at[h * GY + s],
                send_sem=ysend.at[h * GY + s], recv_sem=yrecv.at[h * GY + s],
                device_id={"gy": s}, device_id_type=MESH,
            ).wait_recv()
        for s in range(GY):
            rows = parts[pl.ds(h * GY + s, 1), HK : HK + 16, :][0].astype(F32)
            square = jnp.concatenate([rows, jnp.zeros((W - 16, W), F32)], axis=0).T
            scale = square[:, 1:2]
            total = total + parts[pl.ds(h * GY + s, 1), 0:HK, :][0].astype(F32) * power(scale)
            tallies = tallies + square
        col = tallies[:, 0:1]
        at = pl.ds(h * (GX // NP), GX // NP)
        scaled[at, :, :] = (total * lax.rsqrt(1.0 + col)).reshape(GX // NP, 8, W)
        pos = poscol[pl.ds(pl.multiple_of(h * HK, HK), HK), :]
        slots_s[...] += jnp.sum(
            jnp.where(pos == iota((HK, KD), 1), col, 0.0), axis=0, keepdims=True
        )

        def range_out(m, carry):
            for i in range(8):
                p = pair_at(gx, i // 2, offset(m)) + i % 2

                @pl.when(p != gx)
                def _():
                    to_range(m * 8 + i, p).start()

            return carry

        lax.fori_loop(h * (8 // NP), (h + 1) * (8 // NP), range_out, 0)
        return carry

    def owners_sent(k, carry):
        to_owner((gx + k) % GX).wait_send()
        return carry

    def ranges_sent(k, carry):
        s = (gx + k) % GX
        to_range(s, s).wait_send()
        return carry

    lax.fori_loop(1, GX, owners_sent, 0)
    lax.fori_loop(0, NP, piece, 0)
    lax.fori_loop(1, GX, ranges_sent, 0)
    moved[pl.ds(gx, 1), :, :] = scaled[pl.ds(56 + gx % 2, 1), :, :]
    slots = slots_s[...]
    slots_ref[...] = jnp.concatenate([slots[:, i * W : (i + 1) * W] for i in range(4)], axis=0)
    tail = hquart[pl.ds(gy, 1), :, :][0]
    for k in range(1, GY):
        s = (gy + GY - k) % GY
        pltpu.make_async_remote_copy(
            src_ref=hquart.at[s], dst_ref=hparts.at[s], send_sem=hsend.at[s],
            recv_sem=hrecv.at[s], device_id={"gy": s}, device_id_type=MESH,
        ).wait_recv()
        tail = tail + hparts[pl.ds(s, 1), :, :][0]

    def finish(k, carry):
        s = (gx + k) % GX
        pltpu.make_async_remote_copy(
            src_ref=scaled.at[s], dst_ref=moved.at[s], send_sem=fsend.at[s],
            recv_sem=frecv.at[s], device_id={"gx": s}, device_id_type=MESH,
        ).wait_recv()
        return carry

    lax.fori_loop(1, GX, finish, 0)
    for k in range(1, GY):
        for h in range(NP):
            to_quarter(h, (gy + k) % GY).wait_send()
        heavy_to((gy + k) % GY).wait_send()

    inputs[4].wait()
    got = moved[...].reshape(KD, W)
    high = got.astype(BF16)
    low = (got - high.astype(F32)).astype(BF16)
    both = dot(place_s[...], jnp.concatenate([high, low], axis=1))
    total = both[:, 0:W] + both[:, W : 2 * W]
    orders = orders_ref[...].astype(F32)
    heavy = tail * lax.rsqrt(1.0 + pltpu.roll(tail, 6, 0))
    line = iota((KD, W), 0)
    reports = []
    for h in range(2):
        ours = iota((1, KD), 1) == 2 * device + h
        key = jnp.sum(jnp.where(ours, hk, 0).astype(F32), axis=1, keepdims=True).astype(I32)
        here = line == key - device * KD
        total = jnp.where(here, heavy[h : h + 1, :], total)
        mine = jnp.sum(jnp.where(here, orders, 0.0), axis=0, keepdims=True)
        reports.append(mine * heavy[h : h + 1, :])
    out_ref[...] = (orders * total).astype(BF16)
    report_ref[...] = jnp.concatenate(reports, axis=0).astype(BF16)


def join(keys, x, ks, heavy_keys, orders):
    rows = x.shape[0]
    chunks = rows // LANES
    dma = pltpu.SemaphoreType.DMA
    return pl.pallas_call(
        join_kernel,
        out_shape=(
            jax.ShapeDtypeStruct((KD, W), BF16),
            jax.ShapeDtypeStruct((2, W), BF16),
            jax.ShapeDtypeStruct((4, W), F32),
        ),
        in_specs=[pl.BlockSpec(memory_space=pl.ANY)] * 5,
        out_specs=(VMEM,) * 3,
        scratch_shapes=[
            pltpu.VMEM(keys.shape, I32),
            pltpu.VMEM(ks.shape, I32),
            pltpu.VMEM(heavy_keys.shape, I32),
            pltpu.VMEM(orders.shape, BF16),
            pltpu.VMEM((528, 512), BF16),
            pltpu.VMEM((chunks, LANES), I32),
            pltpu.VMEM((chunks, LANES), I32),
            pltpu.VMEM((chunks, LANES), I32),
            pltpu.VMEM((chunks, LANES), I32),
            pltpu.VMEM((rows, W), BF16),
            pltpu.VMEM((rows, W), BF16),
            pltpu.VMEM((rows, 2 * W), BF16),
            pltpu.VMEM((512, 256), F32),
            pltpu.VMEM((256, 512), BF16),
            pltpu.VMEM((2, 256, 2 * W), F32),
            pltpu.VMEM((2 * GX + 16, W), F32),
            pltpu.VMEM((GX, W), I32),
            pltpu.VMEM((GX, W), I32),
            pltpu.VMEM((512, W), I32),
            pltpu.VMEM((512, W), I32),
            pltpu.VMEM((GX, MSG, W), I16),
            pltpu.VMEM((GX, MSG, W), I16),
            pltpu.VMEM((512, 2 * W), BF16),
            pltpu.VMEM((8, 512), I32),
            pltpu.VMEM((OWN, 1), I32),
            pltpu.VMEM((OWN, 2 * W), F32),
            pltpu.VMEM((OWN, W), F32),
            pltpu.VMEM((8, W), F32),
            pltpu.VMEM((8, W), F32),
            pltpu.VMEM((NP * GY, HK + 16, W), I16),
            pltpu.VMEM((NP * GY, HK + 16, W), I16),
            pltpu.VMEM((GY, 8, W), F32),
            pltpu.VMEM((GY, 8, W), F32),
            pltpu.VMEM((GX, 8, W), F32),
            pltpu.VMEM((GX, 8, W), F32),
            pltpu.VMEM((KD, KD), BF16),
            pltpu.VMEM((KD, 1), I32),
            pltpu.VMEM((1, KD), F32),
            dma((GX,)), dma((GX,)), dma((NP * GY,)), dma((NP * GY,)), dma((GY,)), dma((GY,)),
            dma((GX,)), dma((GX,)), dma((5,)),
        ],
        compiler_params=pltpu.CompilerParams(
            collective_id=0, has_side_effects=True, vmem_limit_bytes=56 * 2**20
        ),
        name="join_rows",
    )(keys, x, ks, heavy_keys, orders)


def hand_on_kernel(a_ref, b_ref, c_ref, out_a, out_b, out_c):
    out_a[...] = a_ref[...]
    out_b[...] = b_ref[...]
    out_c[...] = c_ref[...]


def hand_on(*arrays):
    return pl.pallas_call(
        hand_on_kernel,
        out_shape=tuple(jax.ShapeDtypeStruct(a.shape, a.dtype) for a in arrays),
        in_specs=[VMEM] * 3,
        out_specs=(VMEM,) * 3,
        name="hand_on",
    )(*arrays)


def body(measures, row_keys, orders, heavy_keys, key_slot):
    result, report, slot_rows = join(
        row_keys.reshape(-1, W), measures, key_slot.reshape(-1, W), heavy_keys.reshape(-1, W), orders
    )
    result, report, slot_rows = hand_on(result, report, slot_rows)
    return (result, report, slot_rows.reshape(KD))


def solution(mesh):
    return jax.shard_map(
        body,
        mesh=mesh,
        in_specs=(P(("gx", "gy"), None), P(("gx", "gy")), P(("gx", "gy"), None), P(), P()),
        out_specs=(P(("gx", "gy"), None), P(("gx", "gy"), None), P(("gx", "gy"))),
        check_vma=False,
    )
```
